32 devices in a mesh: tm: 8 (over y, x, core), space: 4 (over z).
Axes of the slice: x: 2, y: 2, z: 4, core: 2. Of those that a mesh axis runs over, the one named last changes fastest.
Arguments:
- rhs: float32 [16, 1024, 1024], P('tm', 'space'), may hold values from -6 to 6
- guess: float32 [16, 1024, 1024], P('tm', 'space'), may hold values from -6 to 6
- diffusion: float32 [1024, 1024], P('space'), may hold values from 0.2 to 2
Outputs:
- solution: float32 [16, 1024, 1024], P('tm', 'space')
- norms: float32 [6], replicated
The draws below stay inside these ranges and needn't reach their ends.
All inputs are finite; a program needn't handle non-finite values.
Results may differ from the reference program's by a relative error of at most 0.0001.
Values sent between devices are 32-bit elements; how exact they have to be, the bound alone decides.
No kernel may reach another device: no remote copies, remote signals or barrier semaphores. Data moves between devices by JAX's collectives and lax.ppermute only.
A program may use at most 64 MiB of HBM per device.

```python
import math
import jax
import jax.numpy as jnp

NY = 1024
LEVELS = 5
NT = 16
NX = 1024


def levels(own_key, extent, split, smallest, high):
    loudness = 1.0
    for dim, shards_of in split:
        steps = jax.random.uniform(jax.random.fold_in(jax.random.fold_in(own_key, 6), dim), (shards_of,), jnp.float32, smallest / len(split), high / len(split))
        loudness = loudness * jnp.repeat(jnp.exp(steps), extent[dim] // shards_of).reshape((-1,) + (1,) * (len(extent) - 1 - dim))
    return loudness


def centred(rng, dims, spread, limit, pieces=(), held_as=jnp.bfloat16):
    gain = levels(rng, dims, pieces, -0.22, 0.18) if pieces else 1.0
    values = jax.random.normal(rng, dims, jnp.float32) * spread * gain
    return jnp.minimum(jnp.maximum(values, -limit), limit).astype(held_as)


def setup_inputs(seed: int = 0) -> dict:
    streams_of = jax.random.split(jax.random.key(seed), 4)
    rhs = centred(streams_of[0], (NT, NX, NY), 1.0, 6.0, ((0, 8), (1, 4)), jnp.float32)
    guess = centred(streams_of[1], (NT, NX, NY), 1.0, 6.0, ((0, 8), (1, 4)), jnp.float32)
    diffusion = jnp.clip(jnp.exp(math.log(2.0) - 2.3025851 * jax.random.uniform(streams_of[2], (NX, NY), jnp.float32) ** levels(streams_of[2], (NX, NY), ((0, 4),), -0.2, 0.2)), 0.2, 2.0)
    return dict(rhs=rhs, guess=guess, diffusion=diffusion)


def neighbours(field):
    padded = jnp.pad(field, ((0, 0), (1, 1), (1, 1)))
    total = padded[:, 2:, 1:-1] + padded[:, :-2, 1:-1]
    total = total + padded[:, 1:-1, 2:] + padded[:, 1:-1, :-2]
    return total

def residual(field, source, scaled, diag):
    before = jnp.concatenate([jnp.zeros_like(field[:1]), field[:-1]], axis=0)
    image = diag * field - scaled * neighbours(field) - before
    return source - image

def reference(rhs, guess, diffusion):
    damping = 0.8
    cells = rhs.shape[1] * rhs.shape[2]
    squares = []
    sources = [rhs]
    fields = []
    field = guess
    for level in range(LEVELS - 1):
        source = sources[level]
        scaled = 2.0 ** level * diffusion
        diag = 1.0 + 4.0 * scaled
        if level == 0:
            field = field + damping * residual(field, source, scaled, diag) / diag
        else:
            field = damping * source / diag
        resid = residual(field, source, scaled, diag)
        squares.append(jnp.sum(resid * resid))
        fields.append(field)
        sources.append(resid[0::2] + resid[1::2])
    level = LEVELS - 1
    source = sources[level]
    scaled = 2.0 ** level * diffusion
    diag = 1.0 + 4.0 * scaled
    field = damping * source / diag
    field = field + damping * residual(field, source, scaled, diag) / diag
    resid = residual(field, source, scaled, diag)
    squares.append(jnp.sum(resid * resid))
    correction = field
    for level in range(LEVELS - 2, -1, -1):
        scaled = 2.0 ** level * diffusion
        diag = 1.0 + 4.0 * scaled
        field = fields[level] + jnp.repeat(correction, 2, axis=0)
        field = field + damping * residual(field, sources[level], scaled, diag) / diag
        correction = field
    scaled = 1.0 * diffusion
    diag = 1.0 + 4.0 * scaled
    resid = residual(correction, rhs, scaled, diag)
    squares.append(jnp.sum(resid * resid))
    norms = jnp.sqrt(jnp.stack(squares) / cells)
    return (correction, norms)
```

```python
import functools
import jax
import jax.numpy as jnp
from jax import lax
from jax.experimental import pallas as pl
from jax.experimental.pallas import tpu as pltpu
from jax.sharding import PartitionSpec as P

LEVELS = 5
DAMPING = 0.8
KEEP = 1.0 - DAMPING
GROUP = 2 ** (LEVELS - 1)
TEAM = GROUP // 2
HALO = 2 * LEVELS + 1
EDGE = 2
REACH = 2 * LEVELS - 3


def vmem():
    return pl.BlockSpec(memory_space=pltpu.VMEM)


def shape(*dims):
    return jax.ShapeDtypeStruct(dims, jnp.float32)


def kernel_call(body, outs, scratch=(), flops=0, n_in=0, specs=None, grid=()):
    return pl.pallas_call(
        body,
        out_shape=outs,
        grid=grid,
        in_specs=specs or [vmem() for _ in range(n_in)],
        out_specs=[vmem() for _ in outs],
        scratch_shapes=[pltpu.VMEM(dims, jnp.float32) for dims in scratch],
        compiler_params=pltpu.CompilerParams(vmem_limit_bytes=56 * 2**20),
        cost_estimate=pl.CostEstimate(flops=flops, bytes_accessed=flops, transcendentals=0),
    )


def tiles(block):
    lead = block.shape[:-2]
    rows, cells = block.shape[-2:]
    split = block.reshape(*lead, rows // 8, 8, cells // 128, 128)
    return jnp.swapaxes(split, -3, -2).reshape(*lead, rows // 8, cells // 16, 128)


def untiles(block):
    lead = block.shape[:-3]
    groups, wide, _ = block.shape[-3:]
    split = block.reshape(*lead, groups, wide // 8, 8, 128)
    return jnp.swapaxes(split, -3, -2).reshape(*lead, groups * 8, wide * 16)


def masks():
    sub = lax.broadcasted_iota(jnp.int32, (8, 128), 0)
    lane = lax.broadcasted_iota(jnp.int32, (8, 128), 1)
    first = lane == 0
    last = lane == 127
    return first, last, first & (sub == 0), last & (sub == 7)


def beside(row, m):
    first, last, left_end, right_end = m
    left = pltpu.roll(row, 1, 1)
    left = jnp.where(first, pltpu.roll(left, 1, 0), left)
    right = pltpu.roll(row, 127, 1)
    right = jnp.where(last, pltpu.roll(right, 7, 0), right)
    return jnp.where(left_end, 0.0, left) + jnp.where(right_end, 0.0, right)


def around(ref, row, m):
    return beside(ref[row], m) + (ref[row - 1] + ref[row + 1])


def loop(low, high, body, carry=None, unroll=4):
    if carry is None:
        lax.fori_loop(low, high, lambda i, c: (body(i), c)[1], 0, unroll=unroll)
        return None
    return lax.fori_loop(low, high, body, carry, unroll=unroll)


def strided(ref, lead, row_group, k):
    return ref[lead + (row_group, pl.ds(k, 8, stride=8))]


def unpack_rows(src, lead, dst, offset, rows):
    def group(g):
        for k in range(8):
            dst[offset + g * 8 + k] = strided(src, lead, g, k)

    loop(0, rows // 8, group, unroll=2)


def pack_edges(g_top, r_top, d_top, g_end, r_end, d_end, top, end):
    count = g_top.shape[1] * 8

    def row_of(ref, lead, row):
        return strided(ref, lead, row // 8, row % 8)

    refs = [((g_top, (t,)), (g_end, (t,))) for t in range(2)]
    refs += [((r_top, (t,)), (r_end, (t,))) for t in range(2)]
    refs += [((d_top, ()), (d_end, ()))]
    for i, ((a, lead_a), (b, lead_b)) in enumerate(refs):
        for k in range(HALO):
            top[i * HALO + k] = row_of(a, lead_a, k)
            end[i * HALO + k] = row_of(b, lead_b, count - HALO + k)


def first_sweep(guess, rhs, diff, low, high, s_ext, w_ext, send, g0, g1):
    rows = guess.shape[1] * 8
    m = masks()
    unpack_rows(diff, (), s_ext, HALO, rows)
    unpack_rows(guess, (0,), g0, HALO, rows)
    unpack_rows(guess, (1,), g1, HALO, rows)
    for k in range(HALO):
        for dst, i in ((g0, 0), (g1, 1), (s_ext, 4)):
            dst[k] = low[i * HALO + k]
            dst[HALO + rows + k] = high[i * HALO + k]

    def weight(i):
        w_ext[i] = DAMPING / (1.0 + 4.0 * s_ext[i])

    loop(0, rows + 2 * HALO, weight)

    def sweep(i, source):
        return KEEP * g1[i] + w_ext[i] * (source + s_ext[i] * around(g1, i, m) + g0[i])

    def inner(g):
        for k in range(8):
            i = HALO + g * 8 + k
            send[i - 2] = sweep(i, strided(rhs, (1,), g, k))

    loop(0, rows // 8, inner, unroll=1)
    for k in range(2, HALO):
        send[k - 2] = sweep(k, low[3 * HALO + k])
    for k in range(0, HALO - 2):
        i = HALO + rows + k
        send[i - 2] = sweep(i, high[3 * HALO + k])
    tail = rows + 2 * (HALO - 2)
    for k in range(HALO - 1):
        send[tail + k] = g1[1 + k]
        send[tail + HALO - 1 + k] = g1[HALO + rows + k]


def local_parts(rhs, low, high, s_ext, w_ext, g0, g1, part0, left0, left1, v1):
    rows = rhs.shape[1] * 8
    m = masks()

    def sweep0(i, source):
        return KEEP * g0[i] + w_ext[i] * (source + s_ext[i] * around(g0, i, m))

    def sweep1(i, source):
        return KEEP * g1[i] + w_ext[i] * (source + s_ext[i] * around(g1, i, m) + g0[i])

    def fill(i, a, b):
        part0[i] = sweep0(i, a)
        v1[i] = sweep1(i, b)

    def inner(g):
        for k in range(8):
            fill(HALO + g * 8 + k, strided(rhs, (0,), g, k), strided(rhs, (1,), g, k))

    loop(0, rows // 8, inner, unroll=1)
    for k in range(1, HALO):
        fill(k, low[2 * HALO + k], low[3 * HALO + k])
    for k in range(0, HALO - 1):
        fill(HALO + rows + k, high[2 * HALO + k], high[3 * HALO + k])

    def rest(i, a, b):
        s = s_ext[i]
        diag = 1.0 + 4.0 * s
        left0[i] = a - diag * part0[i] + s * around(part0, i, m)
        left1[i] = b - diag * v1[i] + s * around(v1, i, m) + part0[i]

    def inner2(g):
        for k in range(8):
            rest(HALO + g * 8 + k, strided(rhs, (0,), g, k), strided(rhs, (1,), g, k))

    loop(0, rows // 8, inner2, unroll=1)
    for k in range(2, HALO):
        rest(k, low[2 * HALO + k], low[3 * HALO + k])
    for k in range(0, HALO - 2):
        rest(HALO + rows + k, high[2 * HALO + k], high[3 * HALO + k])


def windows_of(rows):
    piece = -(-(rows + 2 * EDGE) // TEAM)
    spare = rows + 2 * EDGE - piece
    starts = [-EDGE + j * spare // (TEAM - 1) for j in range(TEAM)]
    return piece, piece + 2 * REACH, starts


def join_first(starts, window, g_prev, got, s_ext, w_ext, part0, left0, left1, v1, out, base0, base1, back, norm, y, coarse):
    rows = g_prev.shape[0] * 8
    m = masks()
    tail = rows + 2 * (HALO - 2)

    def inner(g):
        for k in range(8):
            i = HALO + g * 8 + k
            y[i] = w_ext[i] * strided(g_prev, (), g, k)

    loop(0, rows // 8, inner, unroll=1)
    for k in range(HALO - 1):
        i = 1 + k
        y[i] = w_ext[i] * got[tail + k]
        i = HALO + rows + k
        y[i] = w_ext[i] * got[tail + HALO - 1 + k]

    def resid(i):
        s = s_ext[i]
        here = y[i]
        a = left0[i] - (1.0 + 4.0 * s) * here + s * around(y, i, m) + got[i - 2]
        return a, left1[i] + here

    def edge(i):
        a, b = resid(i)
        coarse[i] = a + b
        return a, b

    def based(i, a, b):
        w = w_ext[i]
        base0[i - HALO + 1] = part0[i] + y[i] + w * a
        value = v1[i] + w * b
        base1[i - HALO + 1] = value
        return value

    def main(i, acc):
        a, b = edge(i)
        back[i - HALO] = based(i, a, b)
        return acc + (a * a + b * b)

    norm[...] = loop(HALO, HALO + rows, main, jnp.zeros((8, 128), jnp.float32))
    for i in (HALO - 1, HALO + rows):
        a, b = edge(i)
        based(i, a, b)
    for i in list(range(2, HALO - 1)) + list(range(HALO + rows + 1, 2 * HALO + rows - 2)):
        edge(i)
    for j, start in enumerate(starts):
        low = start - REACH + HALO

        def copy(i, j=j, low=low):
            out[j, i] = coarse[low + i]

        loop(0, window, copy)


def coarse_levels(starts, rows, where, g_in, s_ext, out, norms, s_win, w_win, v_ref, e_ref, *bases):
    window = g_in.shape[1]
    piece = window - 2 * REACH
    m = masks()
    place = where[0]
    start = -EDGE + place * (rows + 2 * EDGE - piece) // (TEAM - 1) - REACH
    first_own = place * (rows // TEAM) - start
    last_own = first_own + rows // TEAM

    def level_weights(i):
        s = s_ext[start + HALO + i]
        s_win[i] = s
        for level in range(1, LEVELS):
            w_win[level - 1, i] = DAMPING / (1.0 + 4.0 * 2.0**level * s)

    loop(0, window, level_weights, unroll=2)

    def own(i):
        return jnp.where((i >= first_own) & (i < last_own), 1.0, 0.0).astype(jnp.float32)

    source = g_in
    zero = jnp.zeros((8, 128), jnp.float32)
    for level in range(1, LEVELS - 1):
        points = TEAM >> (level - 1)
        lost = level - 1
        base = bases[2 * (level - 1)]
        target = bases[2 * (level - 1) + 1]

        def smooth(i, level=level, points=points, source=source):
            w = w_win[level - 1, i]
            for p in range(points):
                v_ref[p, i] = w * source[p, i]

        loop(lost, window - lost, smooth, unroll=2)

        def descend(i, acc, level=level, points=points, source=source, base=base, target=target):
            s = 2.0**level * s_win[i]
            w = w_win[level - 1, i]
            pairs = []
            total = zero
            before = None
            for p in range(points):
                here = v_ref[p, i]
                r = KEEP * source[p, i] + s * (beside(here, m) + (v_ref[p, i - 1] + v_ref[p, i + 1]))
                if before is not None:
                    r = r + before
                base[p, i] = here + w * r
                total = total + r * r
                pairs.append(r)
                before = here
            for q in range(points // 2):
                target[q, i] = pairs[2 * q] + pairs[2 * q + 1]
            return acc + own(i) * total

        norms[level - 1] = loop(lost + 1, window - lost - 1, descend, zero, unroll=1)
        source = target

    level = LEVELS - 1
    lost = level - 1

    def smooth_last(i):
        v_ref[0, i] = w_win[level - 1, i] * source[0, i]

    loop(lost, window - lost, smooth_last)

    def again(i):
        s = 2.0**level * s_win[i]
        r = KEEP * source[0, i] + s * (beside(v_ref[0, i], m) + (v_ref[0, i - 1] + v_ref[0, i + 1]))
        e_ref[0, i] = v_ref[0, i] + w_win[level - 1, i] * r

    loop(lost + 1, window - lost - 1, again)

    def last_residual(i, acc):
        s = 2.0**level * s_win[i]
        here = e_ref[0, i]
        r = source[0, i] - (1.0 + 4.0 * s) * here
        r = r + s * (beside(here, m) + (e_ref[0, i - 1] + e_ref[0, i + 1]))
        return acc + own(i) * (r * r)

    norms[level - 1] = loop(lost + 2, window - lost - 2, last_residual, zero)

    lost = LEVELS - 1
    field, other = e_ref, v_ref
    for level in range(LEVELS - 2, 0, -1):
        points = TEAM >> (level - 1)
        lost += 1
        base = bases[2 * (level - 1)]

        def ascend(i, level=level, points=points, base=base, field=field, other=other):
            s = 2.0**level * s_win[i]
            w = w_win[level - 1, i]
            before = None
            for q in range(points // 2):
                e = field[q, i]
                part = KEEP * e + w * (s * (beside(e, m) + (field[q, i - 1] + field[q, i + 1])))
                kept = w * e
                for p in (2 * q, 2 * q + 1):
                    value = base[p, i] + part
                    drift = before if p == 2 * q else kept
                    if drift is not None:
                        value = value + drift
                    if level == 1:
                        out[p, i - REACH] = value
                        if p + 1 < points:
                            out[p + 1, i - REACH + piece] = value
                    else:
                        other[p, i] = value
                before = kept

        loop(lost, window - lost, ascend, unroll=1)
        field, other = other, field

    def blank(i):
        out[0, piece + i] = zero

    loop(0, piece, blank)


def finish(starts, piece, got, rhs, s_ext, w_ext, base0, base1, back, norm0, norms, out, sums, e, before, sol0, sol1):
    rows = rhs.shape[1] * 8
    m = masks()
    for j, start in enumerate(starts):

        def copy(i, j=j, start=start):
            e[start + EDGE + i] = got[j, i]
            before[start + EDGE + i] = got[j, piece + i]

        loop(0, piece, copy)

    def correct(i):
        s = s_ext[i + HALO - 1]
        w = w_ext[i + HALO - 1]
        here = e[i + 1]
        part = KEEP * here + w * (s * around(e, i + 1, m))
        sol0[i] = base0[i] + part + w * before[i + 1]
        sol1[i] = base1[i] + part + w * here

    loop(0, rows + 2, correct)

    def last(g, acc):
        for k in range(8):
            i = g * 8 + k
            s = s_ext[i + HALO]
            w = w_ext[i + HALO]
            diag = 1.0 + 4.0 * s
            past = before[i + EDGE]
            past = back[i] + KEEP * past + w * (s * around(before, i + EDGE, m) + past)
            a = sol0[i + 1]
            b = sol1[i + 1]
            ra = strided(rhs, (0,), g, k) - diag * a + s * around(sol0, i + 1, m) + past
            rb = strided(rhs, (1,), g, k) - diag * b + s * around(sol1, i + 1, m) + a
            out[0, g, pl.ds(k, 8, stride=8)] = a
            out[1, g, pl.ds(k, 8, stride=8)] = b
            acc = acc + (ra * ra + rb * rb)
        return acc

    final = loop(0, rows // 8, last, jnp.zeros((8, 128), jnp.float32), unroll=1)
    parts = [norm0[...]] + [norms[k] for k in range(LEVELS - 1)] + [final]
    for k, part in enumerate(parts):
        sums[pl.ds(k, 1)] = jnp.sum(part, axis=0, keepdims=True)
    for k in range(len(parts), 8):
        sums[pl.ds(k, 1)] = jnp.zeros((1, 128), jnp.float32)


def coarse_plain(g_in, s_win, own, earlier):
    cells = g_in.shape[-2] * 128

    def flat(x):
        return x.reshape(*x.shape[:-2], cells)

    def around_plain(v):
        padded = jnp.pad(v, ((0, 0), (1, 1), (1, 1)))
        total = padded[:, 2:, 1:-1] + padded[:, :-2, 1:-1]
        return total + padded[:, 1:-1, 2:] + padded[:, 1:-1, :-2]

    def resid(v, g, s, before):
        past = jnp.concatenate([before, v[:-1]], axis=0)
        return g - (1.0 + 4.0 * s) * v + s * around_plain(v) + past

    source = flat(g_in)
    s_win = flat(s_win)
    sources, fields, norms = [], [], []
    for level in range(1, LEVELS):
        s = 2.0**level * s_win
        w = DAMPING / (1.0 + 4.0 * s)
        v = w * source
        r = resid(v, source, s, earlier(v[-1:]))
        if level == LEVELS - 1:
            v = v + w * r
            r = resid(v, source, s, earlier(v[-1:]))
        masked = jnp.where(own[None, :, None], r, 0.0)
        norms.append((masked * masked).reshape(-1, 8, 128).sum(0))
        sources.append(source)
        fields.append(v)
        if level < LEVELS - 1:
            source = r[0::2] + r[1::2]
    field = fields[-1]
    for level in range(LEVELS - 2, 0, -1):
        s = 2.0**level * s_win
        w = DAMPING / (1.0 + 4.0 * s)
        field = fields[level - 1] + jnp.repeat(field, 2, axis=0)
        field = field + w * resid(field, sources[level - 1], s, earlier(field[-1:]))
    past = jnp.concatenate([earlier(field[-1:]), field[:-1]], axis=0)
    both = [x[:, REACH : x.shape[1] - REACH] for x in (field, past)]
    both = jnp.concatenate(both, axis=1)
    return both.reshape(*both.shape[:2], 8, 128), jnp.stack(norms)


def body(count, strips, rhs, guess, diffusion):
    points, rows, cells = rhs.shape
    assert points == 2 and cells == 1024 and count % TEAM == 0
    assert rows % (8 * TEAM) == 0
    total_cells = rows * strips * cells
    groups = rows // 8
    piece, window, starts = windows_of(rows)
    wide = cells // 16
    ext = rows + 2 * HALO
    up = [(i, i + 1) for i in range(strips - 1)]
    down = [(i + 1, i) for i in range(strips - 1)]
    later = [(i, i + 1) for i in range(count - 1)]

    rhs_t, guess_t, diff_t = tiles(rhs), tiles(guess), tiles(diffusion)
    edge_groups = -(-HALO // 8)
    assert groups % edge_groups == 0
    far = groups // edge_groups - 1

    def edge_specs(block):
        time = pl.BlockSpec((2, edge_groups, wide, 128), lambda i: (0, block, 0, 0))
        flat = pl.BlockSpec((edge_groups, wide, 128), lambda i: (block, 0, 0))
        return [time, time, flat]

    top, end = kernel_call(
        pack_edges, [shape(5 * HALO, 8, 128)] * 2, specs=edge_specs(0) + edge_specs(far), grid=(1,)
    )(guess_t, rhs_t, diff_t, guess_t, rhs_t, diff_t)
    low = lax.ppermute(end, "space", up)
    high = lax.ppermute(top, "space", down)
    g_prev = tiles(lax.ppermute(guess[1], "tm", later))

    sent = rows + 2 * (HALO - 2) + 2 * (HALO - 1)
    s_ext, w_ext, send, g0, g1 = kernel_call(
        first_sweep,
        [shape(ext, 8, 128), shape(ext, 8, 128), shape(sent, 8, 128), shape(ext, 8, 128), shape(ext, 8, 128)],
        n_in=5,
    )(guess_t, rhs_t, diff_t, low, high)
    got = lax.ppermute(send, "tm", later)
    part0, left0, left1, v1 = kernel_call(local_parts, [shape(ext, 8, 128)] * 4, n_in=7, flops=10**7)(
        rhs_t, low, high, s_ext, w_ext, g0, g1
    )
    mine, base0, base1, back, norm0 = kernel_call(
        functools.partial(join_first, starts, window),
        [shape(TEAM, window, 8, 128), shape(rows + 2, 8, 128), shape(rows + 2, 8, 128), shape(rows, 8, 128), shape(8, 128)],
        scratch=[(ext, 8, 128)] * 2,
        n_in=8,
    )(g_prev, got, s_ext, w_ext, part0, left0, left1, v1)

    teams = [list(range(k, k + TEAM)) for k in range(0, count, TEAM)]

    def exchange(x):
        return lax.all_to_all(x, "tm", 0, 0, axis_index_groups=teams if len(teams) > 1 else None)

    g_win = exchange(mine)
    g_win, back = lax.optimization_barrier((g_win, back))
    back = lax.ppermute(back, "tm", later)
    place = lax.axis_index("tm") % TEAM
    if len(teams) == 1:
        half = [(TEAM >> level, window, 8, 128) for level in range(LEVELS)]
        bases = []
        for level in range(1, LEVELS - 1):
            bases += [half[level - 1], half[level]]
        fields, norms = kernel_call(
            functools.partial(coarse_levels, starts, rows),
            [shape(TEAM, 2 * piece, 8, 128), shape(LEVELS - 1, 8, 128)],
            scratch=[(window, 8, 128), (LEVELS - 1, window, 8, 128), half[0], half[0]] + bases,
            specs=[pl.BlockSpec(memory_space=pltpu.SMEM), vmem(), vmem()],
        )(place.astype(jnp.int32).reshape(1), g_win, s_ext)
    else:
        start = -EDGE + place * (rows + 2 * EDGE - piece) // (TEAM - 1) - REACH
        s_win = lax.dynamic_slice_in_dim(s_ext, start + HALO, window, axis=0)
        at = start + jnp.arange(window) - place * (rows // TEAM)
        own = (at >= 0) & (at < rows // TEAM)
        jumps = [(i, i + TEAM) for i in range(count - TEAM)]
        fields, norms = coarse_plain(g_win, s_win, own, lambda v: lax.ppermute(v, "tm", jumps))
    fields = exchange(fields)

    out, sums = kernel_call(
        functools.partial(finish, starts, piece),
        [shape(2, groups, wide, 128), shape(8, 128)],
        scratch=[(rows + 2 * EDGE, 8, 128)] * 2 + [(rows + 2, 8, 128)] * 2,
        n_in=9,
    )(fields, rhs_t, s_ext, w_ext, base0, base1, back, norm0, norms)

    every = jnp.broadcast_to(sums[None], (count * strips, 8, 128))
    every = lax.all_to_all(every, ("tm", "space"), 0, 0)
    totals = every.sum(axis=(0, 2))[: LEVELS + 1]
    return untiles(out), jnp.sqrt(totals / total_cells)


def solution(mesh):
    in_specs = (P("tm", "space", None), P("tm", "space", None), P("space", None))
    out_specs = (P("tm", "space", None), P())
    step = functools.partial(body, mesh.shape["tm"], mesh.shape["space"])
    return jax.shard_map(step, mesh=mesh, in_specs=in_specs, out_specs=out_specs, check_vma=False)
```

```python
import functools
import math
import jax
import jax.numpy as jnp
from jax import lax
from jax.experimental import pallas as pl
from jax.experimental.pallas import tpu as pltpu
from jax.sharding import PartitionSpec as P

LEVELS = 5
DAMPING = 0.8
KEEP = 1.0 - DAMPING
GROUP = 2 ** (LEVELS - 1)
TEAM = GROUP // 2
HALO = 2 * LEVELS + 1
EDGE = 2
REACH = 2 * LEVELS - 3


def vmem():
    return pl.BlockSpec(memory_space=pltpu.VMEM)


def shape(*dims):
    return jax.ShapeDtypeStruct(dims, jnp.float32)


def kept(*dims):
    return pltpu.VMEM(dims, jnp.float32)


def keep(*arrays):
    return [pltpu.with_memory_space_constraint(x, pltpu.VMEM) for x in arrays]


def kernel_call(body, outs, scratch=(), flops=0, n_in=0, specs=None, grid=()):
    def call(*args):
        held = sum(math.prod(dims) for dims in scratch)
        held += sum(math.prod(x.shape) for x in list(outs) + list(args))
        return pl.pallas_call(
            body,
            out_shape=outs,
            grid=grid,
            in_specs=specs or [vmem() for _ in range(n_in)],
            out_specs=[vmem() for _ in outs],
            scratch_shapes=[pltpu.VMEM(dims, jnp.float32) for dims in scratch],
            compiler_params=pltpu.CompilerParams(vmem_limit_bytes=4 * held + 2**21),
            cost_estimate=pl.CostEstimate(flops=flops, bytes_accessed=flops, transcendentals=0),
        )(*args)

    return call


def tiles(block):
    lead = block.shape[:-2]
    rows, cells = block.shape[-2:]
    split = block.reshape(*lead, rows // 8, 8, cells // 128, 128)
    return jnp.swapaxes(split, -3, -2).reshape(*lead, rows // 8, cells // 16, 128)


def untiles(block):
    lead = block.shape[:-3]
    groups, wide, _ = block.shape[-3:]
    split = block.reshape(*lead, groups, wide // 8, 8, 128)
    return jnp.swapaxes(split, -3, -2).reshape(*lead, groups * 8, wide * 16)


def masks():
    sub = lax.broadcasted_iota(jnp.int32, (8, 128), 0)
    lane = lax.broadcasted_iota(jnp.int32, (8, 128), 1)
    first = lane == 0
    last = lane == 127
    return first, last, first & (sub == 0), last & (sub == 7)


def beside(row, m):
    first, last, left_end, right_end = m
    left = pltpu.roll(row, 1, 1)
    left = jnp.where(first, pltpu.roll(left, 1, 0), left)
    right = pltpu.roll(row, 127, 1)
    right = jnp.where(last, pltpu.roll(right, 7, 0), right)
    return jnp.where(left_end, 0.0, left) + jnp.where(right_end, 0.0, right)


def around(ref, row, m):
    return beside(ref[row], m) + (ref[row - 1] + ref[row + 1])


def loop(low, high, body, carry=None, unroll=4):
    quiet = carry is None
    steps = (high - low) // unroll

    def block(n, value):
        for k in range(unroll):
            value = (body(low + n * unroll + k), value)[1] if quiet else body(low + n * unroll + k, value)
        return value

    value = lax.fori_loop(0, steps, block, 0 if quiet else carry)
    for i in range(low + steps * unroll, high):
        value = (body(i), value)[1] if quiet else body(i, value)
    return None if quiet else value


BLOCK = 32


def padded(rows):
    return -(-(rows - 2) // BLOCK) * BLOCK + 2


def block_loop(low, high, body, carry, unroll):
    high = low + -(-(high - low) // unroll) * unroll
    return loop(low, high, body, carry, unroll)


def strided(ref, lead, row_group, k):
    return ref[lead + (row_group, pl.ds(k, 8, stride=8))]


def place_of():
    return lax.rem(lax.axis_index("tm"), TEAM)


def odd_strip():
    return lax.rem(lax.axis_index("space"), 2) == 1


def either(flag, body, one, two):
    pl.when(flag)(lambda: body(two, one))
    pl.when(jnp.logical_not(flag))(lambda: body(one, two))


def pack_edges(g_top, r_top, d_top, g_end, r_end, d_end, pair, other):
    count = g_top.shape[1] * 8
    refs = [((g_top, (t,)), (g_end, (t,))) for t in range(2)]
    refs += [((r_top, (t,)), (r_end, (t,))) for t in range(2)]
    refs += [((d_top, ()), (d_end, ()))]

    def fill(end, top):
        for i, ((a, lead_a), (b, lead_b)) in enumerate(refs):
            for k in range(HALO):
                top[i * HALO + k] = strided(a, lead_a, k // 8, k % 8)
                row = count - HALO + k
                end[i * HALO + k] = strided(b, lead_b, row // 8, row % 8)

    either(odd_strip(), fill, pair, other)


def first_sweep(guess, rhs, diff, pair, other, s_ext, w_ext, send, g0, g1, low, high):
    rows = guess.shape[1] * 8
    m = masks()

    def unpack(g):
        for k in range(8):
            i = HALO + g * 8 + k
            s = strided(diff, (), g, k)
            s_ext[i] = s
            w_ext[i] = DAMPING / (1.0 + 4.0 * s)
            g0[i] = strided(guess, (0,), g, k)
            g1[i] = strided(guess, (1,), g, k)

    def order(after, before):
        for k in range(5 * HALO):
            low[k] = before[k]
            high[k] = after[k]

    either(odd_strip(), order, pair, other)
    loop(0, rows // 8, unpack, unroll=2)
    for k in range(HALO):
        for dst, i in ((g0, 0), (g1, 1), (s_ext, 4)):
            dst[k] = low[i * HALO + k]
            dst[HALO + rows + k] = high[i * HALO + k]
        for i in (k, HALO + rows + k):
            w_ext[i] = DAMPING / (1.0 + 4.0 * s_ext[i])

    def sweep(i, source):
        return KEEP * g1[i] + w_ext[i] * (source + s_ext[i] * around(g1, i, m) + g0[i])

    def inner(g):
        for k in range(8):
            i = HALO + g * 8 + k
            send[i - 2] = sweep(i, strided(rhs, (1,), g, k))

    loop(0, rows // 8, inner, unroll=4)
    for k in range(2, HALO):
        send[k - 2] = sweep(k, low[3 * HALO + k])
    for k in range(0, HALO - 2):
        i = HALO + rows + k
        send[i - 2] = sweep(i, high[3 * HALO + k])
    tail = rows + 2 * (HALO - 2)
    for k in range(HALO - 1):
        send[tail + k] = g1[1 + k]
        send[tail + HALO - 1 + k] = g1[HALO + rows + k]


def local_parts(rhs, low, high, s_ext, w_ext, g0, g1, part0, left0, left1, v1):
    rows = rhs.shape[1] * 8
    m = masks()

    def sweep0(i, source):
        return KEEP * g0[i] + w_ext[i] * (source + s_ext[i] * around(g0, i, m))

    def sweep1(i, source):
        return KEEP * g1[i] + w_ext[i] * (source + s_ext[i] * around(g1, i, m) + g0[i])

    def fill(i, a, b):
        part0[i] = sweep0(i, a)
        v1[i] = sweep1(i, b)

    def inner(g):
        for k in range(8):
            fill(HALO + g * 8 + k, strided(rhs, (0,), g, k), strided(rhs, (1,), g, k))

    loop(0, rows // 8, inner, unroll=2)
    for k in range(1, HALO):
        fill(k, low[2 * HALO + k], low[3 * HALO + k])
    for k in range(0, HALO - 1):
        fill(HALO + rows + k, high[2 * HALO + k], high[3 * HALO + k])

    def rest(i, a, b):
        s = s_ext[i]
        diag = 1.0 + 4.0 * s
        left0[i] = a - diag * part0[i] + s * around(part0, i, m)
        left1[i] = b - diag * v1[i] + s * around(v1, i, m) + part0[i]

    def inner2(g):
        for k in range(8):
            rest(HALO + g * 8 + k, strided(rhs, (0,), g, k), strided(rhs, (1,), g, k))

    loop(0, rows // 8, inner2, unroll=2)
    for k in range(2, HALO):
        rest(k, low[2 * HALO + k], low[3 * HALO + k])
    for k in range(0, HALO - 2):
        rest(HALO + rows + k, high[2 * HALO + k], high[3 * HALO + k])


def windows_of(rows):
    piece = -(-(rows + 2 * EDGE) // TEAM)
    spare = rows + 2 * EDGE - piece

    def start(j):
        return j * spare // (TEAM - 1) - EDGE

    return piece, piece + 2 * REACH, start


def join_first(start_of, window, g_prev, got, s_ext, w_ext, part0, left0, left1, v1, *refs):
    outs = refs[:TEAM]
    base0, base1, back, norm, y, coarse = refs[TEAM:]
    place = place_of()
    rows = g_prev.shape[0] * 8
    m = masks()
    tail = rows + 2 * (HALO - 2)

    def inner(g):
        for k in range(8):
            i = HALO + g * 8 + k
            y[i] = w_ext[i] * strided(g_prev, (), g, k)

    loop(0, rows // 8, inner, unroll=2)
    for k in range(HALO - 1):
        i = 1 + k
        y[i] = w_ext[i] * got[tail + k]
        i = HALO + rows + k
        y[i] = w_ext[i] * got[tail + HALO - 1 + k]

    def resid(i):
        s = s_ext[i]
        here = y[i]
        a = left0[i] - (1.0 + 4.0 * s) * here + s * around(y, i, m) + got[i - 2]
        return a, left1[i] + here

    def edge(i):
        a, b = resid(i)
        coarse[i] = a + b
        return a, b

    def based(i, a, b):
        w = w_ext[i]
        base0[i - HALO + 1] = part0[i] + y[i] + w * a
        value = v1[i] + w * b
        base1[i - HALO + 1] = value
        return value

    def main(i, acc):
        a, b = edge(i)
        back[i - HALO] = based(i, a, b)
        return acc + (a * a + b * b)

    norm[...] = loop(HALO, HALO + rows, main, jnp.zeros((8, 128), jnp.float32), unroll=32)
    for i in (HALO - 1, HALO + rows):
        a, b = edge(i)
        based(i, a, b)
    for i in list(range(2, HALO - 1)) + list(range(HALO + rows + 1, 2 * HALO + rows - 2)):
        edge(i)
    for k, out in enumerate(outs):
        low = start_of(place ^ k) - REACH + HALO

        def copy(i, out=out, low=low):
            out[i] = coarse[low + i]

        loop(0, window, copy, unroll=16)


def coarse_levels(start_of, rows, s_ext, *refs):
    g_in, refs = refs[:TEAM], refs[TEAM:]
    outs, refs = refs[:TEAM], refs[TEAM:]
    norms, s_win, w_win, v_ref, e_ref, final = refs[:6]
    bases = refs[6:]
    window = g_in[0].shape[0]
    piece = window - 2 * REACH
    m = masks()
    place = place_of()
    start = start_of(place) - REACH
    first_own = place * (rows // TEAM) - start
    last_own = first_own + rows // TEAM

    def level_weights(i):
        s = s_ext[start + HALO + i]
        s_win[i] = s
        for level in range(1, LEVELS):
            w_win[level - 1, i] = DAMPING / (1.0 + 4.0 * 2.0**level * s)

    loop(0, window, level_weights, unroll=4)

    def own(i, value):
        return jnp.where((i >= first_own) & (i < last_own), value, 0.0)

    source = None
    zero = jnp.zeros((8, 128), jnp.float32)
    for level in range(1, LEVELS - 1):
        points = TEAM >> (level - 1)
        lost = level - 1
        base = bases[2 * (level - 1)]
        target = bases[2 * (level - 1) + 1]

        def smooth(i, level=level, points=points, source=source):
            w = w_win[level - 1, i]
            for p in range(points):
                if source is None:
                    v_ref[place ^ p, i] = w * g_in[p][i]
                else:
                    v_ref[p, i] = w * source[p, i]

        loop(0, window, smooth, unroll=4)

        def descend(i, acc, level=level, points=points, source=source, base=base, target=target):
            s = 2.0**level * s_win[i]
            w = w_win[level - 1, i]
            pairs = []
            total = zero
            before = None
            for p in range(points):
                here = v_ref[p, i]
                r = 0.25 * here + s * (here + beside(here, m) + (v_ref[p, i - 1] + v_ref[p, i + 1]))
                if before is not None:
                    r = r + before
                base[p, i] = here + w * r
                total = total + r * r
                pairs.append(r)
                before = here
            for q in range(points // 2):
                target[q, i] = pairs[2 * q] + pairs[2 * q + 1]
            return acc + own(i, total)

        norms[level - 1] = block_loop(1, window - 1, descend, zero, BLOCK // points)
        source = target

    level = LEVELS - 1
    lost = level - 1

    def smooth_last(i):
        v_ref[0, i] = w_win[level - 1, i] * source[0, i]

    loop(0, window, smooth_last, unroll=16)

    def again(i):
        s = 2.0**level * s_win[i]
        here = v_ref[0, i]
        r = 0.25 * here + s * (here + beside(here, m) + (v_ref[0, i - 1] + v_ref[0, i + 1]))
        e_ref[0, i] = here + w_win[level - 1, i] * r

    block_loop(1, window - 1, again, None, BLOCK)

    def last_residual(i, acc):
        s = 2.0**level * s_win[i]
        here = e_ref[0, i]
        r = source[0, i] - (1.0 + 4.0 * s) * here
        r = r + s * (beside(here, m) + (e_ref[0, i - 1] + e_ref[0, i + 1]))
        return acc + own(i, r * r)

    norms[level - 1] = block_loop(1, window - 1, last_residual, zero, BLOCK)

    lost = LEVELS - 1
    field, other = e_ref, v_ref
    for level in range(LEVELS - 2, 0, -1):
        points = TEAM >> (level - 1)
        lost += 1
        base = bases[2 * (level - 1)]

        def ascend(i, level=level, points=points, base=base, field=field, other=other):
            s = 2.0**level * s_win[i]
            w = w_win[level - 1, i]
            before = None
            for q in range(points // 2):
                e = field[q, i]
                part = KEEP * e + w * (s * (beside(e, m) + (field[q, i - 1] + field[q, i + 1])))
                kept = w * e
                for p in (2 * q, 2 * q + 1):
                    value = base[p, i] + part
                    drift = before if p == 2 * q else kept
                    if drift is not None:
                        value = value + drift
                    if level == 1:
                        final[p + 1, i - REACH] = value
                    else:
                        other[p, i] = value
                before = kept

        span = BLOCK // points * 2
        if level == 1:
            loop(lost, window - lost, ascend, unroll=min(8, span))
        else:
            block_loop(1, window - 1, ascend, None, span)
        field, other = other, field

    def blank(i):
        final[0, i] = zero

    loop(0, piece, blank, unroll=11)
    for k, out in enumerate(outs):

        def copy(i, k=k, out=out):
            out[i] = final[(place ^ k) + 1, i]
            out[piece + i] = final[place ^ k, i]

        loop(0, piece, copy, unroll=11)


def finish(start_of, piece, rhs, s_ext, w_ext, base0, base1, back, norm0, norms, *refs):
    fields = refs[:TEAM]
    out, sums, e, before, sol0, sol1 = refs[TEAM:]
    rows = rhs.shape[1] * 8
    m = masks()
    place = place_of()
    for k, got in enumerate(fields):
        start = start_of(place ^ k) + EDGE

        def copy(i, got=got, start=start):
            e[start + i] = got[i]
            before[start + i] = got[piece + i]

        loop(0, piece, copy, unroll=11)

    def correct(i):
        s = s_ext[i + HALO - 1]
        w = w_ext[i + HALO - 1]
        here = e[i + 1]
        part = KEEP * here + w * (s * around(e, i + 1, m))
        sol0[i] = base0[i] + part + w * before[i + 1]
        sol1[i] = base1[i] + part + w * here

    loop(0, rows + 2, correct, unroll=24)

    def last(g, acc):
        for k in range(8):
            i = g * 8 + k
            s = s_ext[i + HALO]
            w = w_ext[i + HALO]
            diag = 1.0 + 4.0 * s
            past = before[i + EDGE]
            past = back[i] + KEEP * past + w * (s * around(before, i + EDGE, m) + past)
            a = sol0[i + 1]
            b = sol1[i + 1]
            ra = strided(rhs, (0,), g, k) - diag * a + s * around(sol0, i + 1, m) + past
            rb = strided(rhs, (1,), g, k) - diag * b + s * around(sol1, i + 1, m) + a
            out[0, g, pl.ds(k, 8, stride=8)] = a
            out[1, g, pl.ds(k, 8, stride=8)] = b
            acc = acc + (ra * ra + rb * rb)
        return acc

    final = loop(0, rows // 8, last, jnp.zeros((8, 128), jnp.float32), unroll=2)
    parts = [norm0[...]] + [norms[k] for k in range(LEVELS - 1)] + [final]
    for k, part in enumerate(parts):
        sums[pl.ds(k, 1)] = jnp.sum(part, axis=0, keepdims=True)
    for k in range(len(parts), 8):
        sums[pl.ds(k, 1)] = jnp.zeros((1, 128), jnp.float32)


def coarse_plain(g_in, s_win, own, earlier):
    cells = g_in.shape[-2] * 128

    def flat(x):
        return x.reshape(*x.shape[:-2], cells)

    def around_plain(v):
        padded = jnp.pad(v, ((0, 0), (1, 1), (1, 1)))
        total = padded[:, 2:, 1:-1] + padded[:, :-2, 1:-1]
        return total + padded[:, 1:-1, 2:] + padded[:, 1:-1, :-2]

    def resid(v, g, s, before):
        past = jnp.concatenate([before, v[:-1]], axis=0)
        return g - (1.0 + 4.0 * s) * v + s * around_plain(v) + past

    source = flat(g_in)
    s_win = flat(s_win)
    sources, fields, norms = [], [], []
    for level in range(1, LEVELS):
        s = 2.0**level * s_win
        w = DAMPING / (1.0 + 4.0 * s)
        v = w * source
        r = resid(v, source, s, earlier(v[-1:]))
        if level == LEVELS - 1:
            v = v + w * r
            r = resid(v, source, s, earlier(v[-1:]))
        masked = jnp.where(own[None, :, None], r, 0.0)
        norms.append((masked * masked).reshape(-1, 8, 128).sum(0))
        sources.append(source)
        fields.append(v)
        if level < LEVELS - 1:
            source = r[0::2] + r[1::2]
    field = fields[-1]
    for level in range(LEVELS - 2, 0, -1):
        s = 2.0**level * s_win
        w = DAMPING / (1.0 + 4.0 * s)
        field = fields[level - 1] + jnp.repeat(field, 2, axis=0)
        field = field + w * resid(field, sources[level - 1], s, earlier(field[-1:]))
    past = jnp.concatenate([earlier(field[-1:]), field[:-1]], axis=0)
    both = [x[:, REACH : x.shape[1] - REACH] for x in (field, past)]
    both = jnp.concatenate(both, axis=1)
    return both.reshape(*both.shape[:2], 8, 128), jnp.stack(norms)


def body(count, strips, rhs, guess, diffusion):
    points, rows, cells = rhs.shape
    assert points == 2 and cells == 1024 and count % TEAM == 0
    assert rows % (8 * TEAM) == 0
    total_cells = rows * strips * cells
    groups = rows // 8
    piece, window, start_of = windows_of(rows)
    wide = cells // 16
    ext = rows + 2 * HALO

    def both(first):
        pairs = [(i, i + 1) for i in range(first, strips - 1, 2)]
        return pairs + [(b, a) for a, b in pairs]

    later = [(i, i + 1) for i in range(count - 1)]

    rhs_t, guess_t, diff_t = tiles(rhs), tiles(guess), tiles(diffusion)
    edge_groups = -(-HALO // 8)
    assert groups % edge_groups == 0
    far = groups // edge_groups - 1

    def edge_specs(block):
        time = pl.BlockSpec((2, edge_groups, wide, 128), lambda i: (0, block, 0, 0))
        flat = pl.BlockSpec((edge_groups, wide, 128), lambda i: (block, 0, 0))
        return [time, time, flat]

    g_prev = tiles(lax.ppermute(guess[1], "tm", later))
    far_args = [pltpu.with_memory_space_constraint(x, pltpu.HBM) for x in (guess_t, rhs_t, diff_t)]
    facing, backing = kernel_call(
        pack_edges, [shape(5 * HALO, 8, 128)] * 2, specs=edge_specs(0) + edge_specs(far), grid=(1,)
    )(*far_args, *far_args)
    facing = lax.ppermute(facing, "space", both(0))
    backing = lax.ppermute(backing, "space", both(1))

    sent = rows + 2 * (HALO - 2) + 2 * (HALO - 1)
    s_ext, w_ext, send, g0, g1, low, high = kernel_call(
        first_sweep,
        [kept(ext, 8, 128)] * 2 + [shape(sent, 8, 128)] + [shape(ext, 8, 128)] * 2 + [shape(5 * HALO, 8, 128)] * 2,
        n_in=5,
    )(guess_t, rhs_t, diff_t, facing, backing)
    got = lax.ppermute(send, "tm", later)
    part0, left0, left1, v1 = kernel_call(local_parts, [shape(ext, 8, 128)] * 4, n_in=7, flops=10**7)(
        rhs_t, low, high, s_ext, w_ext, g0, g1
    )
    *mine, base0, base1, back, norm0 = kernel_call(
        functools.partial(join_first, start_of, window),
        [shape(window, 8, 128)] * TEAM
        + [kept(rows + 2, 8, 128), kept(rows + 2, 8, 128), shape(rows, 8, 128), shape(8, 128)],
        scratch=[(ext, 8, 128)] * 2,
        n_in=8,
    )(g_prev, got, s_ext, w_ext, part0, left0, left1, v1)

    def exchange(parts):
        moved = [parts[0]]
        for k in range(1, TEAM):
            moved.append(lax.ppermute(parts[k], "tm", [(i, i ^ k) for i in range(count)]))
        return moved

    mine = exchange(mine)
    *mine, back = lax.optimization_barrier((*mine, back))
    back = lax.ppermute(back, "tm", later)
    if count == TEAM:
        tall = padded(window)
        half = [(TEAM >> level, tall, 8, 128) for level in range(LEVELS)]
        bases = []
        for level in range(1, LEVELS - 1):
            bases += [half[level - 1], half[level]]
        *fields, norms = kernel_call(
            functools.partial(coarse_levels, start_of, rows),
            [shape(2 * piece, 8, 128)] * TEAM + [shape(LEVELS - 1, 8, 128)],
            scratch=[(tall, 8, 128), (LEVELS - 1, tall, 8, 128), half[0], half[0], (TEAM + 1, piece, 8, 128)] + bases,
            n_in=1 + TEAM,
        )(s_ext, *mine)
    else:
        place = place_of()
        order = place ^ jnp.arange(TEAM)
        start = start_of(place) - REACH
        s_win = lax.dynamic_slice_in_dim(s_ext, start + HALO, window, axis=0)
        at = start + jnp.arange(window) - place * (rows // TEAM)
        own = (at >= 0) & (at < rows // TEAM)
        jumps = [(i, i + TEAM) for i in range(count - TEAM)]
        fields, norms = coarse_plain(jnp.stack(mine)[order], s_win, own, lambda v: lax.ppermute(v, "tm", jumps))
        fields = list(fields[order])
    fields = exchange(fields)

    s_ext, w_ext, base0, base1 = keep(s_ext, w_ext, base0, base1)
    out, sums = kernel_call(
        functools.partial(finish, start_of, piece),
        [shape(2, groups, wide, 128), shape(8, 128)],
        scratch=[(rows + 2 * EDGE, 8, 128)] * 2 + [(rows + 2, 8, 128)] * 2,
        n_in=8 + TEAM,
    )(rhs_t, s_ext, w_ext, base0, base1, back, norm0, norms, *fields)

    every = jnp.broadcast_to(sums[None], (count * strips, 8, 128))
    every = lax.all_to_all(every, ("tm", "space"), 0, 0)
    totals = every.sum(axis=(0, 2))[: LEVELS + 1]
    return untiles(out), jnp.sqrt(totals / total_cells)


def solution(mesh):
    in_specs = (P("tm", "space", None), P("tm", "space", None), P("space", None))
    out_specs = (P("tm", "space", None), P())
    step = functools.partial(body, mesh.shape["tm"], mesh.shape["space"])
    step = jax.shard_map(step, mesh=mesh, in_specs=in_specs, out_specs=out_specs, check_vma=False)
    return step
```

```python
import functools
import math
import jax
import jax.numpy as jnp
from jax import lax
from jax.experimental import pallas as pl
from jax.experimental.pallas import tpu as pltpu
from jax.sharding import PartitionSpec as P

LEVELS = 5
DAMPING = 0.8
KEEP = 1.0 - DAMPING
GROUP = 2 ** (LEVELS - 1)
TEAM = GROUP // 2
SWAPS = (2, 6, 4, 3, 7, 5, 1)
HALO = 2 * LEVELS + 1
SIDE = HALO - 1
EDGE = 2
REACH = 2 * LEVELS - 3


def vmem():
    return pl.BlockSpec(memory_space=pltpu.VMEM)


def shape(*dims):
    return jax.ShapeDtypeStruct(dims, jnp.float32)


def kept(*dims):
    return pltpu.VMEM(dims, jnp.float32)


def keep(*arrays):
    return [pltpu.with_memory_space_constraint(x, pltpu.VMEM) for x in arrays]


def kernel_call(body, outs, scratch=(), flops=0, n_in=0, specs=None, grid=(), more=()):
    def call(*args):
        held = sum(math.prod(dims) for dims in scratch)
        held += sum(math.prod(x.shape) for x in list(outs) + list(args))
        return pl.pallas_call(
            body,
            out_shape=outs,
            grid=grid,
            in_specs=specs or [vmem() for _ in range(n_in)],
            out_specs=[vmem() for _ in outs],
            scratch_shapes=[pltpu.VMEM(dims, jnp.float32) for dims in scratch] + list(more),
            compiler_params=pltpu.CompilerParams(vmem_limit_bytes=4 * held + 2**21),
            cost_estimate=pl.CostEstimate(flops=flops, bytes_accessed=flops, transcendentals=0),
        )(*args)

    return call


def tiles(block):
    lead = block.shape[:-2]
    rows, cells = block.shape[-2:]
    split = block.reshape(*lead, rows // 8, 8, cells // 128, 128)
    return jnp.swapaxes(split, -3, -2).reshape(*lead, rows // 8, cells // 16, 128)


def untiles(block):
    lead = block.shape[:-3]
    groups, wide, _ = block.shape[-3:]
    split = block.reshape(*lead, groups, wide // 8, 8, 128)
    return jnp.swapaxes(split, -3, -2).reshape(*lead, groups * 8, wide * 16)


def masks():
    sub = lax.broadcasted_iota(jnp.int32, (8, 128), 0)
    lane = lax.broadcasted_iota(jnp.int32, (8, 128), 1)
    first = lane == 0
    last = lane == 127
    return first, last, first & (sub == 0), last & (sub == 7)


def beside(row, m):
    first, last, left_end, right_end = m
    left = pltpu.roll(row, 1, 1)
    left = jnp.where(first, pltpu.roll(left, 1, 0), left)
    right = pltpu.roll(row, 127, 1)
    right = jnp.where(last, pltpu.roll(right, 7, 0), right)
    return jnp.where(left_end, 0.0, left) + jnp.where(right_end, 0.0, right)


def around(ref, row, m):
    return beside(ref[row], m) + (ref[row - 1] + ref[row + 1])


def loop(low, high, body, carry=None, unroll=4):
    quiet = carry is None
    steps = (high - low) // unroll

    def block(n, value):
        for k in range(unroll):
            value = (body(low + n * unroll + k), value)[1] if quiet else body(low + n * unroll + k, value)
        return value

    value = lax.fori_loop(0, steps, block, 0 if quiet else carry)
    for i in range(low + steps * unroll, high):
        value = (body(i), value)[1] if quiet else body(i, value)
    return None if quiet else value


BLOCK = 64


def padded(rows):
    return -(-(rows - 2) // BLOCK) * BLOCK + 2


def block_loop(low, high, body, carry, unroll):
    high = low + -(-(high - low) // unroll) * unroll
    return loop(low, high, body, carry, unroll)


def strided(ref, lead, row_group, k):
    return ref[lead + (row_group, pl.ds(k, 8, stride=8))]


def place_of():
    return lax.rem(lax.axis_index("tm"), TEAM)


def odd_strip():
    return lax.rem(lax.axis_index("space"), 2) == 1


def either(flag, body, one, two):
    pl.when(flag)(lambda: body(two, one))
    pl.when(jnp.logical_not(flag))(lambda: body(one, two))


def pack_edges(guess, g_top, r_top, d_top, g_end, r_end, d_end, pair, other, later, done):
    copy = pltpu.make_async_copy(guess.at[1], later, done)
    copy.start()
    count = g_top.shape[1] * 8
    refs = [((g_top, (t,)), (g_end, (t,))) for t in range(2)]
    refs += [((r_top, (t,)), (r_end, (t,))) for t in range(2)]
    refs += [((d_top, ()), (d_end, ()))]

    def fill(end, top):
        for i, ((a, lead_a), (b, lead_b)) in enumerate(refs):
            for k in range(HALO):
                top[i * HALO + k] = strided(a, lead_a, k // 8, k % 8)
                row = count - HALO + k
                end[i * HALO + k] = strided(b, lead_b, row // 8, row % 8)

    either(odd_strip(), fill, pair, other)
    copy.wait()


def first_sweep(guess, rhs, diff, send, g1):
    rows = guess.shape[1] * 8
    m = masks()

    def unpack(g):
        for k in range(8):
            i = g * 8 + k
            g1[1 + i] = strided(guess, (1,), g, k)

    loop(0, rows // 8, unpack, unroll=2)

    def sweep(g):
        for k in range(8):
            i = g * 8 + k
            s = strided(diff, (), g, k)
            w = DAMPING / (1.0 + 4.0 * s)
            whole = strided(rhs, (1,), g, k) + s * around(g1, 1 + i, m) + strided(guess, (0,), g, k)
            send[i] = KEEP * g1[1 + i] + w * whole

    loop(0, rows // 8, sweep, unroll=4)


def local_parts(guess, rhs, diff, pair, other, s_ext, w_ext, part0, left0, left1, v1, edges, g0, g1, low, high):
    rows = rhs.shape[1] * 8
    m = masks()

    def unpack(g):
        for k in range(8):
            i = HALO + g * 8 + k
            s = strided(diff, (), g, k)
            s_ext[i] = s
            w_ext[i] = DAMPING / (1.0 + 4.0 * s)
            g0[i] = strided(guess, (0,), g, k)
            g1[i] = strided(guess, (1,), g, k)

    def order(after, before):
        for k in range(5 * HALO):
            low[k] = before[k]
            high[k] = after[k]

    either(odd_strip(), order, pair, other)
    loop(0, rows // 8, unpack, unroll=2)
    for k in range(HALO):
        for dst, i in ((g0, 0), (g1, 1), (s_ext, 4)):
            dst[k] = low[i * HALO + k]
            dst[HALO + rows + k] = high[i * HALO + k]
        for i in (k, HALO + rows + k):
            w_ext[i] = DAMPING / (1.0 + 4.0 * s_ext[i])

    def fill(i, a, b):
        s = s_ext[i]
        w = w_ext[i]
        part0[i] = KEEP * g0[i] + w * (a + s * around(g0, i, m))
        v1[i] = KEEP * g1[i] + w * (b + s * around(g1, i, m) + g0[i])

    def inner(g):
        for k in range(8):
            fill(HALO + g * 8 + k, strided(rhs, (0,), g, k), strided(rhs, (1,), g, k))

    loop(0, rows // 8, inner, unroll=2)
    for k in range(1, HALO):
        fill(k, low[2 * HALO + k], low[3 * HALO + k])
    for k in range(0, HALO - 1):
        fill(HALO + rows + k, high[2 * HALO + k], high[3 * HALO + k])
    for k in range(SIDE):
        edges[k] = v1[2 + k]
        edges[SIDE + k] = v1[HALO + rows - 1 + k]
        edges[2 * SIDE + k] = g1[1 + k]
        edges[3 * SIDE + k] = g1[HALO + rows + k]

    def rest(i, a, b):
        s = s_ext[i]
        diag = 1.0 + 4.0 * s
        left0[i] = a - diag * part0[i] + s * around(part0, i, m)
        left1[i] = b - diag * v1[i] + s * around(v1, i, m) + part0[i]

    def inner2(g):
        for k in range(8):
            rest(HALO + g * 8 + k, strided(rhs, (0,), g, k), strided(rhs, (1,), g, k))

    loop(0, rows // 8, inner2, unroll=2)
    for k in range(2, HALO):
        rest(k, low[2 * HALO + k], low[3 * HALO + k])
    for k in range(0, HALO - 2):
        rest(HALO + rows + k, high[2 * HALO + k], high[3 * HALO + k])


def windows_of(rows):
    piece = -(-(rows + 2 * EDGE) // TEAM)
    spare = rows + 2 * EDGE - piece

    def start(j):
        return j * spare // (TEAM - 1) - EDGE

    return piece, piece + 2 * REACH, start


def join_first(start_of, window, g_prev, got, edges, s_ext, w_ext, part0, left0, left1, v1, *refs):
    outs = refs[:TEAM]
    base0, base1, back1, back2, norm, y, coarse = refs[TEAM:]
    place = place_of()
    rows = got.shape[0]
    m = masks()

    def inner(g):
        for k in range(8):
            i = HALO + g * 8 + k
            y[i] = w_ext[i] * strided(g_prev, (), g, k)

    loop(0, rows // 8, inner, unroll=2)
    for k in range(SIDE):
        y[1 + k] = w_ext[1 + k] * edges[2 * SIDE + k]
        i = HALO + rows + k
        y[i] = w_ext[i] * edges[3 * SIDE + k]

    def resid(i, swept):
        s = s_ext[i]
        here = y[i]
        a = left0[i] - (1.0 + 4.0 * s) * here + s * around(y, i, m) + swept
        return a, left1[i] + here

    def edge(i, swept):
        a, b = resid(i, swept)
        coarse[i] = a + b
        return a, b

    def based(i, a, b):
        w = w_ext[i]
        base0[i - HALO + 1] = part0[i] + y[i] + w * a
        value = v1[i] + w * b
        base1[i - HALO + 1] = value
        return value

    acc = jnp.zeros((8, 128), jnp.float32)
    first = HALO
    for back in (back1, back2):

        def main(i, acc, back=back, first=first):
            a, b = edge(i, got[i - HALO])
            back[i - first] = based(i, a, b)
            return acc + (a * a + b * b)

        low = max(first, HALO + 1)
        high = min(first + back.shape[0], HALO + rows - 1)
        acc = loop(low, high, main, acc, unroll=32)
        first += back.shape[0]
    for k in range(SIDE):
        for i, at in ((2 + k, k), (HALO + rows - 1 + k, SIDE + k)):
            a, b = edge(i, edges[at])
            if HALO - 1 <= i <= HALO + rows:
                value = based(i, a, b)
            if i == HALO:
                back1[0] = value
                acc = acc + (a * a + b * b)
            if i == HALO + rows - 1:
                back2[back2.shape[0] - 1] = value
                acc = acc + (a * a + b * b)
    norm[...] = acc
    for k, out in enumerate(outs):
        low = start_of(place ^ k) - REACH + HALO

        def copy(i, out=out, low=low):
            out[i] = coarse[low + i]

        loop(0, window, copy, unroll=16)


def coarse_levels(start_of, rows, s_ext, *refs):
    g_in, refs = refs[:TEAM], refs[TEAM:]
    outs, refs = refs[:TEAM], refs[TEAM:]
    norms, s_win, w_win, v_ref, e_ref, final = refs[:6]
    bases = refs[6:]
    window = g_in[0].shape[0]
    piece = window - 2 * REACH
    m = masks()
    place = place_of()
    start = start_of(place) - REACH
    first_own = place * (rows // TEAM) - start
    last_own = first_own + rows // TEAM

    def level_weights(i):
        s = s_ext[start + HALO + i]
        s_win[i] = s
        for level in range(1, LEVELS):
            w_win[level - 1, i] = DAMPING / (1.0 + 4.0 * 2.0**level * s)

    loop(0, window, level_weights, unroll=4)

    def own(i, value):
        return jnp.where((i >= first_own) & (i < last_own), value, 0.0)

    source = None
    zero = jnp.zeros((8, 128), jnp.float32)
    for level in range(1, LEVELS - 1):
        points = TEAM >> (level - 1)
        lost = level - 1
        base = bases[2 * (level - 1)]
        target = bases[2 * (level - 1) + 1]

        def smooth(i, level=level, points=points, source=source):
            w = w_win[level - 1, i]
            for p in range(points):
                if source is None:
                    v_ref[place ^ p, i] = w * g_in[p][i]
                else:
                    v_ref[p, i] = w * source[p, i]

        loop(0, window, smooth, unroll=4)

        def descend(i, acc, level=level, points=points, source=source, base=base, target=target):
            s = 2.0**level * s_win[i]
            w = w_win[level - 1, i]
            pairs = []
            total = zero
            before = None
            for p in range(points):
                here = v_ref[p, i]
                r = 0.25 * here + s * (here + beside(here, m) + (v_ref[p, i - 1] + v_ref[p, i + 1]))
                if before is not None:
                    r = r + before
                base[p, i] = here + w * r
                total = total + r * r
                pairs.append(r)
                before = here
            for q in range(points // 2):
                target[q, i] = pairs[2 * q] + pairs[2 * q + 1]
            return acc + own(i, total)

        norms[level - 1] = block_loop(1, window - 1, descend, zero, BLOCK // points)
        source = target

    level = LEVELS - 1
    lost = level - 1

    def smooth_last(i):
        v_ref[0, i] = w_win[level - 1, i] * source[0, i]

    loop(0, window, smooth_last, unroll=16)

    def again(i):
        s = 2.0**level * s_win[i]
        here = v_ref[0, i]
        r = 0.25 * here + s * (here + beside(here, m) + (v_ref[0, i - 1] + v_ref[0, i + 1]))
        e_ref[0, i] = here + w_win[level - 1, i] * r

    block_loop(1, window - 1, again, None, BLOCK)

    def last_residual(i, acc):
        s = 2.0**level * s_win[i]
        here = e_ref[0, i]
        r = source[0, i] - (1.0 + 4.0 * s) * here
        r = r + s * (beside(here, m) + (e_ref[0, i - 1] + e_ref[0, i + 1]))
        return acc + own(i, r * r)

    norms[level - 1] = block_loop(1, window - 1, last_residual, zero, BLOCK)

    lost = LEVELS - 1
    field, other = e_ref, v_ref
    for level in range(LEVELS - 2, 0, -1):
        points = TEAM >> (level - 1)
        lost += 1
        base = bases[2 * (level - 1)]

        def ascend(i, level=level, points=points, base=base, field=field, other=other):
            s = 2.0**level * s_win[i]
            w = w_win[level - 1, i]
            before = None
            for q in range(points // 2):
                e = field[q, i]
                part = KEEP * e + w * (s * (beside(e, m) + (field[q, i - 1] + field[q, i + 1])))
                kept = w * e
                for p in (2 * q, 2 * q + 1):
                    value = base[p, i] + part
                    drift = before if p == 2 * q else kept
                    if drift is not None:
                        value = value + drift
                    if level == 1:
                        final[p + 1, i - REACH] = value
                    else:
                        other[p, i] = value
                before = kept

        span = BLOCK // points * 2
        if level == 1:
            loop(lost, window - lost, ascend, unroll=min(8, span))
        else:
            block_loop(1, window - 1, ascend, None, span)
        field, other = other, field

    def blank(i):
        final[0, i] = zero

    loop(0, piece, blank, unroll=11)
    for k, out in enumerate(outs):

        def copy(i, k=k, out=out):
            out[i] = final[(place ^ k) + 1, i]
            out[piece + i] = final[place ^ k, i]

        loop(0, piece, copy, unroll=11)


def finish(start_of, piece, rhs, s_ext, w_ext, base0, base1, *refs):
    fields = refs[:TEAM]
    out, left, norm, e, before, sol0, sol1 = refs[TEAM:]
    rows = rhs.shape[1] * 8
    m = masks()
    place = place_of()
    for k, got in enumerate(fields):
        start = start_of(place ^ k) + EDGE

        def copy(i, got=got, start=start):
            e[start + i] = got[i]
            before[start + i] = got[piece + i]

        loop(0, piece, copy, unroll=11)

    def correct(i):
        s = s_ext[i + HALO - 1]
        w = w_ext[i + HALO - 1]
        here = e[i + 1]
        part = KEEP * here + w * (s * around(e, i + 1, m))
        sol0[i] = base0[i] + part + w * before[i + 1]
        sol1[i] = base1[i] + part + w * here

    loop(0, rows + 2, correct, unroll=43)

    def last(g, acc):
        for k in range(8):
            i = g * 8 + k
            s = s_ext[i + HALO]
            w = w_ext[i + HALO]
            diag = 1.0 + 4.0 * s
            past = before[i + EDGE]
            past = KEEP * past + w * (s * around(before, i + EDGE, m) + past)
            a = sol0[i + 1]
            b = sol1[i + 1]
            left[i] = strided(rhs, (0,), g, k) - diag * a + s * around(sol0, i + 1, m) + past
            rb = strided(rhs, (1,), g, k) - diag * b + s * around(sol1, i + 1, m) + a
            out[0, g, pl.ds(k, 8, stride=8)] = a
            out[1, g, pl.ds(k, 8, stride=8)] = b
            acc = acc + rb * rb
        return acc

    norm[...] = loop(0, rows // 8, last, jnp.zeros((8, 128), jnp.float32), unroll=2)


def add_up(left, back1, back2, norm0, norms, norm, sums):
    acc = norm[...]
    first = 0
    for back in (back1, back2):

        def body(i, acc, back=back, first=first):
            r = left[first + i] + back[i]
            return acc + r * r

        acc = loop(0, back.shape[0], body, acc, unroll=16)
        first += back.shape[0]
    parts = [norm0[...]] + [norms[k] for k in range(LEVELS - 1)] + [acc]
    for k, part in enumerate(parts):
        sums[pl.ds(k, 1)] = jnp.sum(part, axis=0, keepdims=True)
    for k in range(len(parts), 8):
        sums[pl.ds(k, 1)] = jnp.zeros((1, 128), jnp.float32)


def coarse_plain(g_in, s_win, own, earlier):
    cells = g_in.shape[-2] * 128

    def flat(x):
        return x.reshape(*x.shape[:-2], cells)

    def around_plain(v):
        padded = jnp.pad(v, ((0, 0), (1, 1), (1, 1)))
        total = padded[:, 2:, 1:-1] + padded[:, :-2, 1:-1]
        return total + padded[:, 1:-1, 2:] + padded[:, 1:-1, :-2]

    def resid(v, g, s, before):
        past = jnp.concatenate([before, v[:-1]], axis=0)
        return g - (1.0 + 4.0 * s) * v + s * around_plain(v) + past

    source = flat(g_in)
    s_win = flat(s_win)
    sources, fields, norms = [], [], []
    for level in range(1, LEVELS):
        s = 2.0**level * s_win
        w = DAMPING / (1.0 + 4.0 * s)
        v = w * source
        r = resid(v, source, s, earlier(v[-1:]))
        if level == LEVELS - 1:
            v = v + w * r
            r = resid(v, source, s, earlier(v[-1:]))
        masked = jnp.where(own[None, :, None], r, 0.0)
        norms.append((masked * masked).reshape(-1, 8, 128).sum(0))
        sources.append(source)
        fields.append(v)
        if level < LEVELS - 1:
            source = r[0::2] + r[1::2]
    field = fields[-1]
    for level in range(LEVELS - 2, 0, -1):
        s = 2.0**level * s_win
        w = DAMPING / (1.0 + 4.0 * s)
        field = fields[level - 1] + jnp.repeat(field, 2, axis=0)
        field = field + w * resid(field, sources[level - 1], s, earlier(field[-1:]))
    past = jnp.concatenate([earlier(field[-1:]), field[:-1]], axis=0)
    both = [x[:, REACH : x.shape[1] - REACH] for x in (field, past)]
    both = jnp.concatenate(both, axis=1)
    return both.reshape(*both.shape[:2], 8, 128), jnp.stack(norms)


def body(count, strips, rhs, guess, diffusion):
    points, rows, cells = rhs.shape
    assert points == 2 and cells == 1024 and count % TEAM == 0
    assert rows % (8 * TEAM) == 0
    total_cells = rows * strips * cells
    groups = rows // 8
    piece, window, start_of = windows_of(rows)
    wide = cells // 16
    ext = rows + 2 * HALO

    def both(first):
        pairs = [(i, i + 1) for i in range(first, strips - 1, 2)]
        return pairs + [(b, a) for a, b in pairs]

    later = [(i, i + 1) for i in range(count - 1)]

    rhs_t, guess_t, diff_t = tiles(rhs), tiles(guess), tiles(diffusion)
    edge_groups = -(-HALO // 8)
    assert groups % edge_groups == 0
    far = groups // edge_groups - 1

    def edge_specs(block):
        time = pl.BlockSpec((2, edge_groups, wide, 128), lambda i: (0, block, 0, 0))
        flat = pl.BlockSpec((edge_groups, wide, 128), lambda i: (block, 0, 0))
        return [time, time, flat]

    far_args = [pltpu.with_memory_space_constraint(x, pltpu.HBM) for x in (guess_t, rhs_t, diff_t)]
    facing, backing, g_prev = kernel_call(
        pack_edges,
        [shape(5 * HALO, 8, 128), shape(5 * HALO, 8, 128), shape(groups, wide, 128)],
        specs=[pl.BlockSpec(memory_space=pl.ANY)] + edge_specs(0) + edge_specs(far),
        grid=(1,),
        more=[pltpu.SemaphoreType.DMA(())],
    )(far_args[0], *far_args, *far_args)
    g_prev = lax.ppermute(g_prev, "tm", later)
    facing = lax.ppermute(facing, "space", both(0))
    backing = lax.ppermute(backing, "space", both(1))
    (send,) = kernel_call(first_sweep, [shape(rows, 8, 128)], scratch=[(rows + 2, 8, 128)], n_in=3)(
        guess_t, rhs_t, diff_t
    )
    got = lax.ppermute(send, "tm", later)
    s_ext, w_ext, part0, left0, left1, v1, edges = kernel_call(
        local_parts,
        [kept(ext, 8, 128)] * 2 + [shape(ext, 8, 128)] * 4 + [shape(4 * SIDE, 8, 128)],
        scratch=[(ext, 8, 128)] * 2 + [(5 * HALO, 8, 128)] * 2,
        n_in=5,
    )(guess_t, rhs_t, diff_t, facing, backing)
    edges = lax.ppermute(edges, "tm", later)
    one = rows * 5 // 80 * 10
    *mine, base0, base1, back1, back2, norm0 = kernel_call(
        functools.partial(join_first, start_of, window),
        [shape(window, 8, 128)] * TEAM
        + [kept(rows + 2, 8, 128)] * 2
        + [shape(one, 8, 128), shape(rows - one, 8, 128), shape(8, 128)],
        scratch=[(ext, 8, 128)] * 2,
        n_in=9,
    )(g_prev, got, edges, s_ext, w_ext, part0, left0, left1, v1)

    def exchange(parts):
        moved = list(parts)
        for k in SWAPS:
            moved[k] = lax.ppermute(parts[k], "tm", [(i, i ^ k) for i in range(count)])
        return moved

    mine = exchange(mine)
    *mine, back1 = lax.optimization_barrier((*mine, back1))
    back1 = lax.ppermute(back1, "tm", later)
    back2 = lax.ppermute(back2, "tm", later)
    if count == TEAM:
        tall = padded(window)
        half = [(TEAM >> level, tall, 8, 128) for level in range(LEVELS)]
        bases = []
        for level in range(1, LEVELS - 1):
            bases += [half[level - 1], half[level]]
        *fields, norms = kernel_call(
            functools.partial(coarse_levels, start_of, rows),
            [shape(2 * piece, 8, 128)] * TEAM + [shape(LEVELS - 1, 8, 128)],
            scratch=[(tall, 8, 128), (LEVELS - 1, tall, 8, 128), half[0], half[0], (TEAM + 1, piece, 8, 128)] + bases,
            n_in=1 + TEAM,
        )(s_ext, *mine)
    else:
        place = place_of()
        order = place ^ jnp.arange(TEAM)
        start = start_of(place) - REACH
        s_win = lax.dynamic_slice_in_dim(s_ext, start + HALO, window, axis=0)
        at = start + jnp.arange(window) - place * (rows // TEAM)
        own = (at >= 0) & (at < rows // TEAM)
        jumps = [(i, i + TEAM) for i in range(count - TEAM)]
        fields, norms = coarse_plain(jnp.stack(mine)[order], s_win, own, lambda v: lax.ppermute(v, "tm", jumps))
        fields = list(fields[order])
    fields = exchange(fields)

    s_ext, w_ext, base0, base1 = keep(s_ext, w_ext, base0, base1)
    out, left, norm = kernel_call(
        functools.partial(finish, start_of, piece),
        [shape(2, groups, wide, 128), shape(rows, 8, 128), shape(8, 128)],
        scratch=[(rows + 2 * EDGE, 8, 128)] * 2 + [(rows + 2, 8, 128)] * 2,
        n_in=5 + TEAM,
    )(rhs_t, s_ext, w_ext, base0, base1, *fields)
    (sums,) = kernel_call(add_up, [shape(8, 128)], n_in=6)(left, back1, back2, norm0, norms, norm)

    every = jnp.broadcast_to(sums[None], (count * strips, 8, 128))
    every = lax.all_to_all(every, ("tm", "space"), 0, 0)
    totals = every.sum(axis=(0, 2))[: LEVELS + 1]
    return untiles(out), jnp.sqrt(totals / total_cells)


def solution(mesh):
    in_specs = (P("tm", "space", None), P("tm", "space", None), P("space", None))
    out_specs = (P("tm", "space", None), P())
    step = functools.partial(body, mesh.shape["tm"], mesh.shape["space"])
    step = jax.shard_map(step, mesh=mesh, in_specs=in_specs, out_specs=out_specs, check_vma=False)
    return step
```

```python
import functools
import math
import jax
import jax.numpy as jnp
from jax import lax
from jax.experimental import pallas as pl
from jax.experimental.pallas import tpu as pltpu
from jax.sharding import PartitionSpec as P

LEVELS = 5
DAMPING = 0.8
KEEP = 1.0 - DAMPING
GROUP = 2 ** (LEVELS - 1)
TEAM = GROUP // 2
DOWN = (2, 6, 4, 3, 7, 5, 1)
UP = (2, 6, 4, 3, 7, 5, 1)
HALO = 2 * LEVELS + 1
SIDE = HALO - 1
EDGE = 2
REACH = 2 * LEVELS - 3


def vmem():
    return pl.BlockSpec(memory_space=pltpu.VMEM)


def shape(*dims):
    return jax.ShapeDtypeStruct(dims, jnp.float32)


def kept(*dims):
    return pltpu.VMEM(dims, jnp.float32)


def keep(*arrays):
    return [pltpu.with_memory_space_constraint(x, pltpu.VMEM) for x in arrays]


def kernel_call(body, outs, scratch=(), flops=0, n_in=0, specs=None, grid=(), more=()):
    def call(*args):
        held = sum(math.prod(dims) for dims in scratch)
        held += sum(math.prod(x.shape) for x in list(outs) + list(args))
        return pl.pallas_call(
            body,
            out_shape=outs,
            grid=grid,
            in_specs=specs or [vmem() for _ in range(n_in)],
            out_specs=[vmem() for _ in outs],
            scratch_shapes=[pltpu.VMEM(dims, jnp.float32) for dims in scratch] + list(more),
            compiler_params=pltpu.CompilerParams(vmem_limit_bytes=4 * held + 2**21),
            cost_estimate=pl.CostEstimate(flops=flops, bytes_accessed=flops, transcendentals=0),
        )(*args)

    return call


def tiles(block):
    lead = block.shape[:-2]
    rows, cells = block.shape[-2:]
    split = block.reshape(*lead, rows // 8, 8, cells // 128, 128)
    return jnp.swapaxes(split, -3, -2).reshape(*lead, rows // 8, cells // 16, 128)


def untiles(block):
    lead = block.shape[:-3]
    groups, wide, _ = block.shape[-3:]
    split = block.reshape(*lead, groups, wide // 8, 8, 128)
    return jnp.swapaxes(split, -3, -2).reshape(*lead, groups * 8, wide * 16)


def masks():
    sub = lax.broadcasted_iota(jnp.int32, (8, 128), 0)
    lane = lax.broadcasted_iota(jnp.int32, (8, 128), 1)
    first = lane == 0
    last = lane == 127
    return first, last, first & (sub == 0), last & (sub == 7)


def beside(row, m):
    first, last, left_end, right_end = m
    left = pltpu.roll(row, 1, 1)
    left = jnp.where(first, pltpu.roll(left, 1, 0), left)
    right = pltpu.roll(row, 127, 1)
    right = jnp.where(last, pltpu.roll(right, 7, 0), right)
    return jnp.where(left_end, 0.0, left) + jnp.where(right_end, 0.0, right)


def around(ref, row, m):
    return beside(ref[row], m) + (ref[row - 1] + ref[row + 1])


def loop(low, high, body, carry=None, unroll=4):
    quiet = carry is None
    steps = (high - low) // unroll

    def block(n, value):
        for k in range(unroll):
            value = (body(low + n * unroll + k), value)[1] if quiet else body(low + n * unroll + k, value)
        return value

    value = lax.fori_loop(0, steps, block, 0 if quiet else carry)
    for i in range(low + steps * unroll, high):
        value = (body(i), value)[1] if quiet else body(i, value)
    return None if quiet else value


BLOCK = 64


def padded(rows):
    return -(-(rows - 2) // BLOCK) * BLOCK + 2


def block_loop(low, high, body, carry, unroll):
    high = low + -(-(high - low) // unroll) * unroll
    return loop(low, high, body, carry, unroll)


def strided(ref, lead, row_group, k):
    return ref[lead + (row_group, pl.ds(k, 8, stride=8))]


def place_of():
    return lax.rem(lax.axis_index("tm"), TEAM)


def odd_strip():
    return lax.rem(lax.axis_index("space"), 2) == 1


def either(flag, body, one, two):
    pl.when(flag)(lambda: body(two, one))
    pl.when(jnp.logical_not(flag))(lambda: body(one, two))


def pack_edges(guess, g_top, r_top, d_top, g_end, r_end, d_end, pair, other, later, done):
    copy = pltpu.make_async_copy(guess.at[1], later, done)
    copy.start()
    count = g_top.shape[1] * 8
    refs = [((g_top, (t,)), (g_end, (t,))) for t in range(2)]
    refs += [((r_top, (t,)), (r_end, (t,))) for t in range(2)]
    refs += [((d_top, ()), (d_end, ()))]

    def fill(end, top):
        for i, ((a, lead_a), (b, lead_b)) in enumerate(refs):
            for k in range(HALO):
                top[i * HALO + k] = strided(a, lead_a, k // 8, k % 8)
                row = count - HALO + k
                end[i * HALO + k] = strided(b, lead_b, row // 8, row % 8)

    either(odd_strip(), fill, pair, other)
    copy.wait()


def first_sweep(guess, rhs, diff, send, g1):
    rows = guess.shape[1] * 8
    m = masks()

    def unpack(g):
        for k in range(8):
            i = g * 8 + k
            g1[1 + i] = strided(guess, (1,), g, k)

    loop(0, rows // 8, unpack, unroll=2)

    def sweep(g):
        for k in range(8):
            i = g * 8 + k
            s = strided(diff, (), g, k)
            w = DAMPING / (1.0 + 4.0 * s)
            whole = strided(rhs, (1,), g, k) + s * around(g1, 1 + i, m) + strided(guess, (0,), g, k)
            send[i] = KEEP * g1[1 + i] + w * whole

    loop(0, rows // 8, sweep, unroll=4)


def local_parts(guess, rhs, diff, pair, other, s_ext, w_ext, part0, left0, left1, v1, edges, g0, g1, low, high):
    rows = rhs.shape[1] * 8
    m = masks()

    def unpack(g):
        for k in range(8):
            i = HALO + g * 8 + k
            s = strided(diff, (), g, k)
            s_ext[i] = s
            w_ext[i] = DAMPING / (1.0 + 4.0 * s)
            g0[i] = strided(guess, (0,), g, k)
            g1[i] = strided(guess, (1,), g, k)

    def order(after, before):
        for k in range(5 * HALO):
            low[k] = before[k]
            high[k] = after[k]

    either(odd_strip(), order, pair, other)
    loop(0, rows // 8, unpack, unroll=2)
    for k in range(HALO):
        for dst, i in ((g0, 0), (g1, 1), (s_ext, 4)):
            dst[k] = low[i * HALO + k]
            dst[HALO + rows + k] = high[i * HALO + k]
        for i in (k, HALO + rows + k):
            w_ext[i] = DAMPING / (1.0 + 4.0 * s_ext[i])

    def fill(i, a, b):
        s = s_ext[i]
        w = w_ext[i]
        part0[i] = KEEP * g0[i] + w * (a + s * around(g0, i, m))
        v1[i] = KEEP * g1[i] + w * (b + s * around(g1, i, m) + g0[i])

    def inner(g):
        for k in range(8):
            fill(HALO + g * 8 + k, strided(rhs, (0,), g, k), strided(rhs, (1,), g, k))

    loop(0, rows // 8, inner, unroll=2)
    for k in range(1, HALO):
        fill(k, low[2 * HALO + k], low[3 * HALO + k])
    for k in range(0, HALO - 1):
        fill(HALO + rows + k, high[2 * HALO + k], high[3 * HALO + k])
    for k in range(SIDE):
        edges[k] = v1[2 + k]
        edges[SIDE + k] = v1[HALO + rows - 1 + k]
        edges[2 * SIDE + k] = g1[1 + k]
        edges[3 * SIDE + k] = g1[HALO + rows + k]

    def rest(i, a, b):
        s = s_ext[i]
        diag = 1.0 + 4.0 * s
        left0[i] = a - diag * part0[i] + s * around(part0, i, m)
        left1[i] = b - diag * v1[i] + s * around(v1, i, m) + part0[i]

    def inner2(g):
        for k in range(8):
            rest(HALO + g * 8 + k, strided(rhs, (0,), g, k), strided(rhs, (1,), g, k))

    loop(0, rows // 8, inner2, unroll=2)
    for k in range(2, HALO):
        rest(k, low[2 * HALO + k], low[3 * HALO + k])
    for k in range(0, HALO - 2):
        rest(HALO + rows + k, high[2 * HALO + k], high[3 * HALO + k])


def windows_of(rows):
    piece = -(-(rows + 2 * EDGE) // TEAM)
    spare = rows + 2 * EDGE - piece

    def start(j):
        return j * spare // (TEAM - 1) - EDGE

    return piece, piece + 2 * REACH, start


def join_first(start_of, window, g_prev, got, edges, s_ext, w_ext, left0, left1, *refs):
    outs = refs[:TEAM]
    y, resid0, coarse = refs[TEAM:]
    place = place_of()
    rows = got.shape[0]
    m = masks()

    def inner(g):
        for k in range(8):
            i = HALO + g * 8 + k
            y[i] = w_ext[i] * strided(g_prev, (), g, k)

    loop(0, rows // 8, inner, unroll=2)
    for k in range(SIDE):
        y[1 + k] = w_ext[1 + k] * edges[2 * SIDE + k]
        i = HALO + rows + k
        y[i] = w_ext[i] * edges[3 * SIDE + k]

    def resid(i, swept):
        s = s_ext[i]
        here = y[i]
        a = left0[i] - (1.0 + 4.0 * s) * here + s * around(y, i, m) + swept
        resid0[i] = a
        coarse[i] = a + left1[i] + here

    loop(HALO + 1, HALO + rows - 1, lambda i: resid(i, got[i - HALO]), unroll=32)
    for k in range(SIDE):
        resid(2 + k, edges[k])
        resid(HALO + rows - 1 + k, edges[SIDE + k])
    for k, out in enumerate(outs):
        low = start_of(place ^ k) - REACH + HALO

        def copy(i, out=out, low=low):
            out[i] = coarse[low + i]

        loop(0, window, copy, unroll=16)


def join_rest(w_ext, part0, left1, v1, y, resid0, base0, base1, back, norm):
    rows = back.shape[0]

    def based(i):
        w = w_ext[i]
        a = resid0[i]
        b = left1[i] + y[i]
        base0[i - HALO + 1] = part0[i] + y[i] + w * a
        value = v1[i] + w * b
        base1[i - HALO + 1] = value
        return a, b, value

    def main(i, acc):
        a, b, value = based(i)
        back[i - HALO] = value
        return acc + (a * a + b * b)

    norm[...] = loop(HALO, HALO + rows, main, jnp.zeros((8, 128), jnp.float32), unroll=8)
    based(HALO - 1)
    based(HALO + rows)


def coarse_levels(start_of, rows, s_ext, *refs):
    g_in, refs = refs[:TEAM], refs[TEAM:]
    outs, refs = refs[:TEAM], refs[TEAM:]
    norms, s_win, w_win, v_ref, e_ref, final = refs[:6]
    bases = refs[6:]
    window = g_in[0].shape[0]
    piece = window - 2 * REACH
    m = masks()
    place = place_of()
    start = start_of(place) - REACH
    first_own = place * (rows // TEAM) - start
    last_own = first_own + rows // TEAM

    def level_weights(i):
        s = s_ext[start + HALO + i]
        s_win[i] = s
        for level in range(1, LEVELS):
            w_win[level - 1, i] = DAMPING / (1.0 + 4.0 * 2.0**level * s)

    loop(0, window, level_weights, unroll=4)

    def own(i, value):
        return jnp.where((i >= first_own) & (i < last_own), value, 0.0)

    source = None
    zero = jnp.zeros((8, 128), jnp.float32)
    for level in range(1, LEVELS - 1):
        points = TEAM >> (level - 1)
        lost = level - 1
        base = bases[2 * (level - 1)]
        target = bases[2 * (level - 1) + 1]

        def smooth(i, level=level, points=points, source=source):
            w = w_win[level - 1, i]
            for p in range(points):
                if source is None:
                    v_ref[place ^ p, i] = w * g_in[p][i]
                else:
                    v_ref[p, i] = w * source[p, i]

        loop(0, window, smooth, unroll=4)

        def descend(i, acc, level=level, points=points, source=source, base=base, target=target):
            s = 2.0**level * s_win[i]
            w = w_win[level - 1, i]
            pairs = []
            total = zero
            before = None
            for p in range(points):
                here = v_ref[p, i]
                r = 0.25 * here + s * (here + beside(here, m) + (v_ref[p, i - 1] + v_ref[p, i + 1]))
                if before is not None:
                    r = r + before
                base[p, i] = here + w * r
                total = total + r * r
                pairs.append(r)
                before = here
            for q in range(points // 2):
                target[q, i] = pairs[2 * q] + pairs[2 * q + 1]
            return acc + own(i, total)

        norms[level - 1] = block_loop(1, window - 1, descend, zero, BLOCK // points)
        source = target

    level = LEVELS - 1
    lost = level - 1

    def smooth_last(i):
        v_ref[0, i] = w_win[level - 1, i] * source[0, i]

    loop(0, window, smooth_last, unroll=16)

    def again(i):
        s = 2.0**level * s_win[i]
        here = v_ref[0, i]
        r = 0.25 * here + s * (here + beside(here, m) + (v_ref[0, i - 1] + v_ref[0, i + 1]))
        e_ref[0, i] = here + w_win[level - 1, i] * r

    block_loop(1, window - 1, again, None, BLOCK)

    def last_residual(i, acc):
        s = 2.0**level * s_win[i]
        here = e_ref[0, i]
        r = source[0, i] - (1.0 + 4.0 * s) * here
        r = r + s * (beside(here, m) + (e_ref[0, i - 1] + e_ref[0, i + 1]))
        return acc + own(i, r * r)

    norms[level - 1] = block_loop(1, window - 1, last_residual, zero, BLOCK)

    lost = LEVELS - 1
    field, other = e_ref, v_ref
    for level in range(LEVELS - 2, 0, -1):
        points = TEAM >> (level - 1)
        lost += 1
        base = bases[2 * (level - 1)]

        def ascend(i, level=level, points=points, base=base, field=field, other=other):
            s = 2.0**level * s_win[i]
            w = w_win[level - 1, i]
            before = None
            for q in range(points // 2):
                e = field[q, i]
                part = KEEP * e + w * (s * (beside(e, m) + (field[q, i - 1] + field[q, i + 1])))
                kept = w * e
                for p in (2 * q, 2 * q + 1):
                    value = base[p, i] + part
                    drift = before if p == 2 * q else kept
                    if drift is not None:
                        value = value + drift
                    if level == 1:
                        final[p + 1, i - REACH] = value
                    else:
                        other[p, i] = value
                before = kept

        span = BLOCK // points * 2
        if level == 1:
            loop(lost, window - lost, ascend, unroll=min(8, span))
        else:
            block_loop(1, window - 1, ascend, None, span)
        field, other = other, field

    def blank(i):
        final[0, i] = zero

    loop(0, piece, blank, unroll=11)
    for k, out in enumerate(outs):

        target = place ^ k
        odd = lax.rem(target, 2)
        half = out.shape[0] - piece

        def copy(i, out=out, at=target + odd):
            out[i] = final[at, i]

        def copy_half(i, out=out, at=target - odd + 1, skip=odd * (piece - half), half=half):
            out[piece + i] = final[at, skip + i]

        loop(0, piece, copy, unroll=11)
        loop(0, half, copy_half, unroll=17)


def odd_place():
    return lax.rem(lax.axis_index("tm"), 2)


def pick_halves(piece, *refs):
    fields, (out,) = refs[:TEAM], refs[TEAM:]
    half = fields[0].shape[0] - piece
    place = place_of()
    for k, got in enumerate(fields):
        first = (place ^ k) * half

        def copy(i, got=got, first=first):
            out[first + i] = got[piece + i]

        loop(0, half, copy, unroll=17)


def spread(field, s_ext, w_ext, out):
    m = masks()

    def body(i):
        s = s_ext[i + HALO - 1]
        out[i] = KEEP * field[i + 1] + w_ext[i + HALO - 1] * (s * around(field, i + 1, m))

    loop(0, out.shape[0], body, unroll=43)


def spread_own(start_of, piece, s_ext, w_ext, *refs):
    fields, (own, out) = refs[:TEAM], refs[TEAM:]
    place = place_of()
    for k, got in enumerate(fields):
        start = start_of(place ^ k) + EDGE

        def copy(i, got=got, start=start):
            own[start + i] = got[i]

        loop(0, piece, copy, unroll=11)
    spread(own, s_ext, w_ext, out)


def finish(start_of, piece, rhs, s_ext, w_ext, base0, base1, own, own_spread, halves, *refs):
    fields = refs[:TEAM]
    out, left, norm, shared, shared_spread, sol0, sol1 = refs[TEAM:]
    rows = rhs.shape[1] * 8
    half = fields[0].shape[0] - piece
    m = masks()
    place = place_of()
    odd = odd_place()
    skip = odd * (piece - half)
    for k, got in enumerate(fields):
        start = start_of(place ^ k) + EDGE + skip

        def copy(i, got=got, start=start):
            shared[start + i] = got[piece + i]

        loop(0, half, copy, unroll=17)
    for j in range(TEAM):
        start = start_of(j) + EDGE + (piece - half) - skip

        def copy(i, j=j, start=start):
            shared[start + i] = halves[j * half + i]

        loop(0, half, copy, unroll=17)
    spread(shared, s_ext, w_ext, shared_spread)

    def solve(now, before):
        e, part = now
        past, past_part = before

        def correct(i):
            w = w_ext[i + HALO - 1]
            sol0[i] = base0[i] + part[i] + w * past[i + 1]
            sol1[i] = base1[i] + part[i] + w * e[i + 1]

        loop(0, rows + 2, correct, unroll=16)

        def last(g, acc):
            for k in range(8):
                i = g * 8 + k
                s = s_ext[i + HALO]
                diag = 1.0 + 4.0 * s
                older = past_part[i + 1] + w_ext[i + HALO] * past[i + EDGE]
                a = sol0[i + 1]
                b = sol1[i + 1]
                left[i] = strided(rhs, (0,), g, k) - diag * a + s * around(sol0, i + 1, m) + older
                rb = strided(rhs, (1,), g, k) - diag * b + s * around(sol1, i + 1, m) + a
                out[0, g, pl.ds(k, 8, stride=8)] = a
                out[1, g, pl.ds(k, 8, stride=8)] = b
                acc = acc + rb * rb
            return acc

        norm[...] = loop(0, rows // 8, last, jnp.zeros((8, 128), jnp.float32), unroll=2)

    either(odd == 1, solve, (shared, shared_spread), (own, own_spread))


def add_up(left, back, norm0, norms, norm, sums):
    def body(i, acc):
        r = left[i] + back[i]
        return acc + r * r

    acc = loop(0, back.shape[0], body, norm[...], unroll=16)
    parts = [norm0[...]] + [norms[k] for k in range(LEVELS - 1)] + [acc]
    for k, part in enumerate(parts):
        sums[pl.ds(k, 1)] = jnp.sum(part, axis=0, keepdims=True)
    for k in range(len(parts), 8):
        sums[pl.ds(k, 1)] = jnp.zeros((1, 128), jnp.float32)


def coarse_plain(g_in, s_win, own, earlier):
    cells = g_in.shape[-2] * 128

    def flat(x):
        return x.reshape(*x.shape[:-2], cells)

    def around_plain(v):
        padded = jnp.pad(v, ((0, 0), (1, 1), (1, 1)))
        total = padded[:, 2:, 1:-1] + padded[:, :-2, 1:-1]
        return total + padded[:, 1:-1, 2:] + padded[:, 1:-1, :-2]

    def resid(v, g, s, before):
        past = jnp.concatenate([before, v[:-1]], axis=0)
        return g - (1.0 + 4.0 * s) * v + s * around_plain(v) + past

    source = flat(g_in)
    s_win = flat(s_win)
    sources, fields, norms = [], [], []
    for level in range(1, LEVELS):
        s = 2.0**level * s_win
        w = DAMPING / (1.0 + 4.0 * s)
        v = w * source
        r = resid(v, source, s, earlier(v[-1:]))
        if level == LEVELS - 1:
            v = v + w * r
            r = resid(v, source, s, earlier(v[-1:]))
        masked = jnp.where(own[None, :, None], r, 0.0)
        norms.append((masked * masked).reshape(-1, 8, 128).sum(0))
        sources.append(source)
        fields.append(v)
        if level < LEVELS - 1:
            source = r[0::2] + r[1::2]
    field = fields[-1]
    for level in range(LEVELS - 2, 0, -1):
        s = 2.0**level * s_win
        w = DAMPING / (1.0 + 4.0 * s)
        field = fields[level - 1] + jnp.repeat(field, 2, axis=0)
        field = field + w * resid(field, sources[level - 1], s, earlier(field[-1:]))
    past = jnp.concatenate([earlier(field[-1:]), field[:-1]], axis=0)
    field, past = [x[:, REACH : x.shape[1] - REACH] for x in (field, past)]
    half = -(-field.shape[1] // 2)
    even = jnp.concatenate([past, field[:, :half]], axis=1)
    odd = jnp.concatenate([field, past[:, -half:]], axis=1)
    both = jnp.where((jnp.arange(TEAM) % 2 == 1)[:, None, None], odd, even)
    return both.reshape(*both.shape[:2], 8, 128), jnp.stack(norms)


def body(count, strips, rhs, guess, diffusion):
    points, rows, cells = rhs.shape
    assert points == 2 and cells == 1024 and count % TEAM == 0
    assert rows % (8 * TEAM) == 0
    total_cells = rows * strips * cells
    groups = rows // 8
    piece, window, start_of = windows_of(rows)
    half_piece = -(-piece // 2)
    wide = cells // 16
    ext = rows + 2 * HALO

    def both(first):
        pairs = [(i, i + 1) for i in range(first, strips - 1, 2)]
        return pairs + [(b, a) for a, b in pairs]

    later = [(i, i + 1) for i in range(count - 1)]

    rhs_t, guess_t, diff_t = tiles(rhs), tiles(guess), tiles(diffusion)
    edge_groups = -(-HALO // 8)
    assert groups % edge_groups == 0
    far = groups // edge_groups - 1

    def edge_specs(block):
        time = pl.BlockSpec((2, edge_groups, wide, 128), lambda i: (0, block, 0, 0))
        flat = pl.BlockSpec((edge_groups, wide, 128), lambda i: (block, 0, 0))
        return [time, time, flat]

    far_args = [pltpu.with_memory_space_constraint(x, pltpu.HBM) for x in (guess_t, rhs_t, diff_t)]
    facing, backing, g_prev = kernel_call(
        pack_edges,
        [shape(5 * HALO, 8, 128), shape(5 * HALO, 8, 128), shape(groups, wide, 128)],
        specs=[pl.BlockSpec(memory_space=pl.ANY)] + edge_specs(0) + edge_specs(far),
        grid=(1,),
        more=[pltpu.SemaphoreType.DMA(())],
    )(far_args[0], *far_args, *far_args)
    g_prev = lax.ppermute(g_prev, "tm", later)
    facing = lax.ppermute(facing, "space", both(0))
    backing = lax.ppermute(backing, "space", both(1))
    (send,) = kernel_call(first_sweep, [shape(rows, 8, 128)], scratch=[(rows + 2, 8, 128)], n_in=3)(
        guess_t, rhs_t, diff_t
    )
    got = lax.ppermute(send, "tm", later)
    s_ext, w_ext, part0, left0, left1, v1, edges = kernel_call(
        local_parts,
        [kept(ext, 8, 128)] * 2 + [shape(ext, 8, 128)] * 4 + [shape(4 * SIDE, 8, 128)],
        scratch=[(ext, 8, 128)] * 2 + [(5 * HALO, 8, 128)] * 2,
        n_in=5,
    )(guess_t, rhs_t, diff_t, facing, backing)
    edges = lax.ppermute(edges, "tm", later)
    *mine, y, resid0 = kernel_call(
        functools.partial(join_first, start_of, window),
        [shape(window, 8, 128)] * TEAM + [shape(ext, 8, 128)] * 2,
        scratch=[(ext, 8, 128)],
        n_in=7,
    )(g_prev, got, edges, s_ext, w_ext, left0, left1)

    def exchange(order, parts):
        moved = list(parts)
        for k in order:
            moved[k] = lax.ppermute(parts[k], "tm", [(i, i ^ k) for i in range(count)])
        return moved

    mine = exchange(DOWN, mine)
    base0, base1, back, norm0 = kernel_call(
        join_rest,
        [kept(rows + 2, 8, 128)] * 2 + [shape(rows, 8, 128), shape(8, 128)],
        n_in=6,
    )(w_ext, part0, left1, v1, y, resid0)
    back = lax.ppermute(back, "tm", later)
    if count == TEAM:
        tall = padded(window)
        half = [(TEAM >> level, tall, 8, 128) for level in range(LEVELS)]
        bases = []
        for level in range(1, LEVELS - 1):
            bases += [half[level - 1], half[level]]
        *fields, norms = kernel_call(
            functools.partial(coarse_levels, start_of, rows),
            [shape(piece + half_piece, 8, 128)] * TEAM + [shape(LEVELS - 1, 8, 128)],
            scratch=[(tall, 8, 128), (LEVELS - 1, tall, 8, 128), half[0], half[0], (TEAM + 1, piece, 8, 128)] + bases,
            n_in=1 + TEAM,
        )(s_ext, *mine)
    else:
        place = place_of()
        order = place ^ jnp.arange(TEAM)
        start = start_of(place) - REACH
        s_win = lax.dynamic_slice_in_dim(s_ext, start + HALO, window, axis=0)
        at = start + jnp.arange(window) - place * (rows // TEAM)
        own = (at >= 0) & (at < rows // TEAM)
        jumps = [(i, i + TEAM) for i in range(count - TEAM)]
        fields, norms = coarse_plain(jnp.stack(mine)[order], s_win, own, lambda v: lax.ppermute(v, "tm", jumps))
        fields = list(fields[order])
    fields = exchange(UP, fields)

    s_ext, w_ext, base0, base1 = keep(s_ext, w_ext, base0, base1)
    (halves,) = kernel_call(
        functools.partial(pick_halves, piece), [shape(TEAM * half_piece, 8, 128)], n_in=TEAM
    )(*fields)
    halves = lax.ppermute(halves, "tm", [(i, i ^ 1) for i in range(count)])
    own, own_spread = kernel_call(
        functools.partial(spread_own, start_of, piece),
        [shape(rows + 2 * EDGE, 8, 128), shape(rows + 2, 8, 128)],
        n_in=2 + TEAM,
    )(s_ext, w_ext, *fields)
    out, left, norm = kernel_call(
        functools.partial(finish, start_of, piece),
        [shape(2, groups, wide, 128), shape(rows, 8, 128), shape(8, 128)],
        scratch=[(rows + 2 * EDGE, 8, 128)] + [(rows + 2, 8, 128)] * 3,
        n_in=8 + TEAM,
    )(rhs_t, s_ext, w_ext, base0, base1, own, own_spread, halves, *fields)
    (sums,) = kernel_call(add_up, [shape(8, 128)], n_in=5)(left, back, norm0, norms, norm)

    every = jnp.broadcast_to(sums[None], (count * strips, 8, 128))
    every = lax.all_to_all(every, ("tm", "space"), 0, 0)
    totals = every.sum(axis=(0, 2))[: LEVELS + 1]
    return untiles(out), jnp.sqrt(totals / total_cells)


def solution(mesh):
    in_specs = (P("tm", "space", None), P("tm", "space", None), P("space", None))
    out_specs = (P("tm", "space", None), P())
    step = functools.partial(body, mesh.shape["tm"], mesh.shape["space"])
    step = jax.shard_map(step, mesh=mesh, in_specs=in_specs, out_specs=out_specs, check_vma=False)
    return step
```

```python
import functools
import math
import jax
import jax.numpy as jnp
from jax import lax
from jax.experimental import pallas as pl
from jax.experimental.pallas import tpu as pltpu
from jax.sharding import PartitionSpec as P

LEVELS = 5
DAMPING = 0.8
KEEP = 1.0 - DAMPING
GROUP = 2 ** (LEVELS - 1)
TEAM = GROUP // 2
DOWN = (2, 6, 4, 3, 7, 5, 1)
UP = (2, 6, 4, 3, 7, 5, 1)
HALO = 2 * LEVELS + 1
SIDE = HALO - 1
EDGE = 2
REACH = 2 * LEVELS - 3


def vmem():
    return pl.BlockSpec(memory_space=pltpu.VMEM)


def shape(*dims):
    return jax.ShapeDtypeStruct(dims, jnp.float32)


def kept(*dims):
    return pltpu.VMEM(dims, jnp.float32)


def keep(*arrays):
    return [pltpu.with_memory_space_constraint(x, pltpu.VMEM) for x in arrays]


def kernel_call(body, outs, scratch=(), flops=0, n_in=0, specs=None, grid=(), more=(), out_specs=None):
    def call(*args):
        held = sum(math.prod(dims) for dims in scratch)
        held += sum(math.prod(x.shape) for x in list(outs) + list(args))
        return pl.pallas_call(
            body,
            out_shape=outs,
            grid=grid,
            in_specs=specs or [vmem() for _ in range(n_in)],
            out_specs=out_specs or [vmem() for _ in outs],
            scratch_shapes=[pltpu.VMEM(dims, jnp.float32) for dims in scratch] + list(more),
            compiler_params=pltpu.CompilerParams(vmem_limit_bytes=4 * held + 2**21),
            cost_estimate=pl.CostEstimate(flops=flops, bytes_accessed=flops, transcendentals=0),
        )(*args)

    return call


def tiles(block):
    lead = block.shape[:-2]
    rows, cells = block.shape[-2:]
    split = block.reshape(*lead, rows // 8, 8, cells // 128, 128)
    return jnp.swapaxes(split, -3, -2).reshape(*lead, rows // 8, cells // 16, 128)


def untiles(block):
    lead = block.shape[:-3]
    groups, wide, _ = block.shape[-3:]
    split = block.reshape(*lead, groups, wide // 8, 8, 128)
    return jnp.swapaxes(split, -3, -2).reshape(*lead, groups * 8, wide * 16)


def masks():
    sub = lax.broadcasted_iota(jnp.int32, (8, 128), 0)
    lane = lax.broadcasted_iota(jnp.int32, (8, 128), 1)
    first = lane == 0
    last = lane == 127
    return first, last, first & (sub == 0), last & (sub == 7)


def beside(row, m):
    first, last, left_end, right_end = m
    left = pltpu.roll(row, 1, 1)
    left = jnp.where(first, pltpu.roll(left, 1, 0), left)
    right = pltpu.roll(row, 127, 1)
    right = jnp.where(last, pltpu.roll(right, 7, 0), right)
    return jnp.where(left_end, 0.0, left) + jnp.where(right_end, 0.0, right)


def around(ref, row, m):
    return beside(ref[row], m) + (ref[row - 1] + ref[row + 1])


def loop(low, high, body, carry=None, unroll=4):
    quiet = carry is None
    steps = (high - low) // unroll

    def block(n, value):
        for k in range(unroll):
            value = (body(low + n * unroll + k), value)[1] if quiet else body(low + n * unroll + k, value)
        return value

    value = lax.fori_loop(0, steps, block, 0 if quiet else carry)
    for i in range(low + steps * unroll, high):
        value = (body(i), value)[1] if quiet else body(i, value)
    return None if quiet else value


BLOCK = 64


def padded(rows):
    return -(-(rows - 2) // BLOCK) * BLOCK + 2


def block_loop(low, high, body, carry, unroll):
    high = low + -(-(high - low) // unroll) * unroll
    return loop(low, high, body, carry, unroll)


def strided(ref, lead, row_group, k):
    return ref[lead + (row_group, pl.ds(k, 8, stride=8))]


def place_of():
    return lax.rem(lax.axis_index("tm"), TEAM)


def odd_strip():
    return lax.rem(lax.axis_index("space"), 2) == 1


def either(flag, body, one, two):
    pl.when(flag)(lambda: body(two, one))
    pl.when(jnp.logical_not(flag))(lambda: body(one, two))


def take_later(guess, out, *done):
    part = out.shape[0] // len(done)
    copies = []
    for k, sem in enumerate(done):
        at = pl.ds(k * part, part)
        copies.append(pltpu.make_async_copy(guess.at[1, at], out.at[at], sem))
    for copy in copies:
        copy.start()
    for copy in copies:
        copy.wait()


def pack_edges(g_top, r_top, d_top, g_end, r_end, d_end, pair, other):
    count = g_top.shape[1] * 8
    refs = [((g_top, (t,)), (g_end, (t,))) for t in range(2)]
    refs += [((r_top, (t,)), (r_end, (t,))) for t in range(2)]
    refs += [((d_top, ()), (d_end, ()))]

    def fill(end, top):
        for i, ((a, lead_a), (b, lead_b)) in enumerate(refs):
            for k in range(HALO):
                top[i * HALO + k] = strided(a, lead_a, k // 8, k % 8)
                row = count - HALO + k
                end[i * HALO + k] = strided(b, lead_b, row // 8, row % 8)

    either(odd_strip(), fill, pair, other)


def first_sweep(guess, rhs, diff, send, g1):
    rows = guess.shape[1] * 8
    m = masks()

    def unpack(g):
        for k in range(8):
            i = g * 8 + k
            g1[1 + i] = strided(guess, (1,), g, k)

    loop(0, rows // 8, unpack, unroll=2)

    def sweep(g):
        for k in range(8):
            i = g * 8 + k
            s = strided(diff, (), g, k)
            w = DAMPING / (1.0 + 4.0 * s)
            whole = strided(rhs, (1,), g, k) + s * around(g1, 1 + i, m) + strided(guess, (0,), g, k)
            send[i] = KEEP * g1[1 + i] + w * whole

    loop(0, rows // 8, sweep, unroll=4)


def local_parts(guess, rhs, diff, pair, other, s_ext, w_ext, part0, left0, left1, v1, edges, g0, g1, low, high):
    rows = rhs.shape[1] * 8
    m = masks()

    def unpack(g):
        for k in range(8):
            i = HALO + g * 8 + k
            s = strided(diff, (), g, k)
            s_ext[i] = s
            w_ext[i] = DAMPING / (1.0 + 4.0 * s)
            g0[i] = strided(guess, (0,), g, k)
            g1[i] = strided(guess, (1,), g, k)

    def order(after, before):
        for k in range(5 * HALO):
            low[k] = before[k]
            high[k] = after[k]

    either(odd_strip(), order, pair, other)
    loop(0, rows // 8, unpack, unroll=2)
    for k in range(HALO):
        for dst, i in ((g0, 0), (g1, 1), (s_ext, 4)):
            dst[k] = low[i * HALO + k]
            dst[HALO + rows + k] = high[i * HALO + k]
        for i in (k, HALO + rows + k):
            w_ext[i] = DAMPING / (1.0 + 4.0 * s_ext[i])

    def fill(i, a, b):
        s = s_ext[i]
        w = w_ext[i]
        part0[i] = KEEP * g0[i] + w * (a + s * around(g0, i, m))
        v1[i] = KEEP * g1[i] + w * (b + s * around(g1, i, m) + g0[i])

    def inner(g):
        for k in range(8):
            fill(HALO + g * 8 + k, strided(rhs, (0,), g, k), strided(rhs, (1,), g, k))

    loop(0, rows // 8, inner, unroll=2)
    for k in range(1, HALO):
        fill(k, low[2 * HALO + k], low[3 * HALO + k])
    for k in range(0, HALO - 1):
        fill(HALO + rows + k, high[2 * HALO + k], high[3 * HALO + k])
    for k in range(SIDE):
        edges[k] = v1[2 + k]
        edges[SIDE + k] = v1[HALO + rows - 1 + k]
        edges[2 * SIDE + k] = g1[1 + k]
        edges[3 * SIDE + k] = g1[HALO + rows + k]

    def rest(i, a, b):
        s = s_ext[i]
        diag = 1.0 + 4.0 * s
        left0[i] = a - diag * part0[i] + s * around(part0, i, m)
        left1[i] = b - diag * v1[i] + s * around(v1, i, m) + part0[i]

    def inner2(g):
        for k in range(8):
            rest(HALO + g * 8 + k, strided(rhs, (0,), g, k), strided(rhs, (1,), g, k))

    loop(0, rows // 8, inner2, unroll=2)
    for k in range(2, HALO):
        rest(k, low[2 * HALO + k], low[3 * HALO + k])
    for k in range(0, HALO - 2):
        rest(HALO + rows + k, high[2 * HALO + k], high[3 * HALO + k])


def windows_of(rows):
    piece = -(-(rows + 2 * EDGE) // TEAM)
    spare = rows + 2 * EDGE - piece

    def start(j):
        return j * spare // (TEAM - 1) - EDGE

    return piece, piece + 2 * REACH, start


def join_first(start_of, window, g_prev, got, edges, s_ext, w_ext, left0, left1, *refs):
    outs = refs[:TEAM]
    y, resid0, coarse = refs[TEAM:]
    place = place_of()
    rows = got.shape[0]
    m = masks()

    def inner(g):
        for k in range(8):
            i = HALO + g * 8 + k
            y[i] = w_ext[i] * strided(g_prev, (), g, k)

    loop(0, rows // 8, inner, unroll=2)
    for k in range(SIDE):
        y[1 + k] = w_ext[1 + k] * edges[2 * SIDE + k]
        i = HALO + rows + k
        y[i] = w_ext[i] * edges[3 * SIDE + k]

    def resid(i, swept):
        s = s_ext[i]
        here = y[i]
        a = left0[i] - (1.0 + 4.0 * s) * here + s * around(y, i, m) + swept
        resid0[i] = a
        coarse[i] = a + left1[i] + here

    loop(HALO + 1, HALO + rows - 1, lambda i: resid(i, got[i - HALO]), unroll=32)
    for k in range(SIDE):
        resid(2 + k, edges[k])
        resid(HALO + rows - 1 + k, edges[SIDE + k])
    for k, out in enumerate(outs):
        low = start_of(place ^ k) - REACH + HALO

        def copy(i, out=out, low=low):
            out[i] = coarse[low + i]

        loop(0, window, copy, unroll=16)


def join_rest(w_ext, part0, left1, v1, y, resid0, base0, base1, back, norm):
    rows = back.shape[0]

    def based(i):
        w = w_ext[i]
        a = resid0[i]
        b = left1[i] + y[i]
        base0[i - HALO + 1] = part0[i] + y[i] + w * a
        value = v1[i] + w * b
        base1[i - HALO + 1] = value
        return a, b, value

    def main(i, acc):
        a, b, value = based(i)
        back[i - HALO] = value
        return acc + (a * a + b * b)

    norm[...] = loop(HALO, HALO + rows, main, jnp.zeros((8, 128), jnp.float32), unroll=8)
    based(HALO - 1)
    based(HALO + rows)


def coarse_levels(start_of, rows, s_ext, *refs):
    g_in, refs = refs[:TEAM], refs[TEAM:]
    outs, refs = refs[:TEAM], refs[TEAM:]
    norms, s_win, w_win, v_ref, e_ref, final = refs[:6]
    bases = refs[6:]
    window = g_in[0].shape[0]
    piece = window - 2 * REACH
    m = masks()
    place = place_of()
    start = start_of(place) - REACH
    first_own = place * (rows // TEAM) - start
    last_own = first_own + rows // TEAM

    def level_weights(i):
        s = s_ext[start + HALO + i]
        s_win[i] = s
        for level in range(1, LEVELS):
            w_win[level - 1, i] = DAMPING / (1.0 + 4.0 * 2.0**level * s)

    loop(0, window, level_weights, unroll=4)

    def own(i, value):
        return jnp.where((i >= first_own) & (i < last_own), value, 0.0)

    source = None
    zero = jnp.zeros((8, 128), jnp.float32)
    for level in range(1, LEVELS - 1):
        points = TEAM >> (level - 1)
        lost = level - 1
        base = bases[2 * (level - 1)]
        target = bases[2 * (level - 1) + 1]

        def smooth(i, level=level, points=points, source=source):
            w = w_win[level - 1, i]
            for p in range(points):
                if source is None:
                    v_ref[place ^ p, i] = w * g_in[p][i]
                else:
                    v_ref[p, i] = w * source[p, i]

        loop(0, window, smooth, unroll=4)

        def descend(i, acc, level=level, points=points, source=source, base=base, target=target):
            s = 2.0**level * s_win[i]
            w = w_win[level - 1, i]
            pairs = []
            total = zero
            before = None
            for p in range(points):
                here = v_ref[p, i]
                r = 0.25 * here + s * (here + beside(here, m) + (v_ref[p, i - 1] + v_ref[p, i + 1]))
                if before is not None:
                    r = r + before
                base[p, i] = here + w * r
                total = total + r * r
                pairs.append(r)
                before = here
            for q in range(points // 2):
                target[q, i] = pairs[2 * q] + pairs[2 * q + 1]
            return acc + own(i, total)

        norms[level - 1] = block_loop(1, window - 1, descend, zero, BLOCK // points)
        source = target

    level = LEVELS - 1
    lost = level - 1

    def smooth_last(i):
        v_ref[0, i] = w_win[level - 1, i] * source[0, i]

    loop(0, window, smooth_last, unroll=16)

    def again(i):
        s = 2.0**level * s_win[i]
        here = v_ref[0, i]
        r = 0.25 * here + s * (here + beside(here, m) + (v_ref[0, i - 1] + v_ref[0, i + 1]))
        e_ref[0, i] = here + w_win[level - 1, i] * r

    block_loop(1, window - 1, again, None, BLOCK)

    def last_residual(i, acc):
        s = 2.0**level * s_win[i]
        here = e_ref[0, i]
        r = source[0, i] - (1.0 + 4.0 * s) * here
        r = r + s * (beside(here, m) + (e_ref[0, i - 1] + e_ref[0, i + 1]))
        return acc + own(i, r * r)

    norms[level - 1] = block_loop(1, window - 1, last_residual, zero, BLOCK)

    lost = LEVELS - 1
    field, other = e_ref, v_ref
    for level in range(LEVELS - 2, 0, -1):
        points = TEAM >> (level - 1)
        lost += 1
        base = bases[2 * (level - 1)]

        def ascend(i, level=level, points=points, base=base, field=field, other=other):
            s = 2.0**level * s_win[i]
            w = w_win[level - 1, i]
            before = None
            for q in range(points // 2):
                e = field[q, i]
                part = KEEP * e + w * (s * (beside(e, m) + (field[q, i - 1] + field[q, i + 1])))
                kept = w * e
                for p in (2 * q, 2 * q + 1):
                    value = base[p, i] + part
                    drift = before if p == 2 * q else kept
                    if drift is not None:
                        value = value + drift
                    if level == 1:
                        final[p + 1, i - REACH] = value
                    else:
                        other[p, i] = value
                before = kept

        span = BLOCK // points * 2
        if level == 1:
            loop(lost, window - lost, ascend, unroll=11)
        else:
            block_loop(1, window - 1, ascend, None, span)
        field, other = other, field

    def blank(i):
        final[0, i] = zero

    loop(0, piece, blank, unroll=11)
    for k, out in enumerate(outs):

        target = place ^ k
        odd = lax.rem(target, 2)
        half = out.shape[0] - piece

        def copy(i, out=out, at=target + odd):
            out[i] = final[at, i]

        def copy_half(i, out=out, at=target - odd + 1, skip=odd * (piece - half), half=half):
            out[piece + i] = final[at, skip + i]

        loop(0, piece, copy, unroll=11)
        loop(0, half, copy_half, unroll=17)


def odd_place():
    return lax.rem(lax.axis_index("tm"), 2)


def pick_halves(piece, *refs):
    fields, (out,) = refs[:TEAM], refs[TEAM:]
    half = fields[0].shape[0] - piece
    place = place_of()
    for k, got in enumerate(fields):
        first = (place ^ k) * half

        def copy(i, got=got, first=first):
            out[first + i] = got[piece + i]

        loop(0, half, copy, unroll=17)


def spread(field, s_ext, w_ext, out):
    m = masks()

    def body(i):
        s = s_ext[i + HALO - 1]
        out[i] = KEEP * field[i + 1] + w_ext[i + HALO - 1] * (s * around(field, i + 1, m))

    loop(0, out.shape[0], body, unroll=43)


def spread_own(start_of, piece, s_ext, w_ext, *refs):
    fields, (own, out) = refs[:TEAM], refs[TEAM:]
    place = place_of()
    for k, got in enumerate(fields):
        start = start_of(place ^ k) + EDGE

        def copy(i, got=got, start=start):
            own[start + i] = got[i]

        loop(0, piece, copy, unroll=11)
    spread(own, s_ext, w_ext, out)


def finish(start_of, piece, rhs, s_ext, w_ext, base0, base1, own, own_spread, halves, *refs):
    fields = refs[:TEAM]
    whole, left, norm, shared, shared_spread, sol0, sol1, out, *done = refs[TEAM:]
    groups = rhs.shape[1]
    share = groups // len(done)
    rows = rhs.shape[1] * 8
    half = fields[0].shape[0] - piece
    m = masks()
    place = place_of()
    odd = odd_place()
    skip = odd * (piece - half)
    for k, got in enumerate(fields):
        start = start_of(place ^ k) + EDGE + skip

        def copy(i, got=got, start=start):
            shared[start + i] = got[piece + i]

        loop(0, half, copy, unroll=17)
    for j in range(TEAM):
        start = start_of(j) + EDGE + (piece - half) - skip

        def copy(i, j=j, start=start):
            shared[start + i] = halves[j * half + i]

        loop(0, half, copy, unroll=17)
    spread(shared, s_ext, w_ext, shared_spread)

    def solve(now, before):
        e, part = now
        past, past_part = before

        def correct(i):
            w = w_ext[i + HALO - 1]
            sol0[i] = base0[i] + part[i] + w * past[i + 1]
            sol1[i] = base1[i] + part[i] + w * e[i + 1]

        loop(0, rows + 2, correct, unroll=16)

        def last(g, acc):
            for k in range(8):
                i = g * 8 + k
                s = s_ext[i + HALO]
                diag = 1.0 + 4.0 * s
                older = past_part[i + 1] + w_ext[i + HALO] * past[i + EDGE]
                a = sol0[i + 1]
                b = sol1[i + 1]
                left[i] = strided(rhs, (0,), g, k) - diag * a + s * around(sol0, i + 1, m) + older
                rb = strided(rhs, (1,), g, k) - diag * b + s * around(sol1, i + 1, m) + a
                out[0, g, pl.ds(k, 8, stride=8)] = a
                out[1, g, pl.ds(k, 8, stride=8)] = b
                acc = acc + rb * rb
            return acc

        acc = jnp.zeros((8, 128), jnp.float32)
        copies = []
        for n, sem in enumerate(done):
            acc = loop(n * share, (n + 1) * share, last, acc, unroll=4)
            at = pl.ds(n * share, share)
            copies.append(pltpu.make_async_copy(out.at[:, at], whole.at[:, at], sem))
            copies[-1].start()
        norm[...] = acc
        for copy in copies:
            copy.wait()

    either(odd == 1, solve, (shared, shared_spread), (own, own_spread))


def add_up(left, back, norm0, norms, norm, sums):
    def body(i, acc):
        r = left[i] + back[i]
        return acc + r * r

    acc = loop(0, back.shape[0], body, norm[...], unroll=16)
    parts = [norm0[...]] + [norms[k] for k in range(LEVELS - 1)] + [acc]
    for k, part in enumerate(parts):
        sums[pl.ds(k, 1)] = jnp.sum(part, axis=0, keepdims=True)
    for k in range(len(parts), 8):
        sums[pl.ds(k, 1)] = jnp.zeros((1, 128), jnp.float32)


def coarse_plain(g_in, s_win, own, earlier):
    cells = g_in.shape[-2] * 128

    def flat(x):
        return x.reshape(*x.shape[:-2], cells)

    def around_plain(v):
        padded = jnp.pad(v, ((0, 0), (1, 1), (1, 1)))
        total = padded[:, 2:, 1:-1] + padded[:, :-2, 1:-1]
        return total + padded[:, 1:-1, 2:] + padded[:, 1:-1, :-2]

    def resid(v, g, s, before):
        past = jnp.concatenate([before, v[:-1]], axis=0)
        return g - (1.0 + 4.0 * s) * v + s * around_plain(v) + past

    source = flat(g_in)
    s_win = flat(s_win)
    sources, fields, norms = [], [], []
    for level in range(1, LEVELS):
        s = 2.0**level * s_win
        w = DAMPING / (1.0 + 4.0 * s)
        v = w * source
        r = resid(v, source, s, earlier(v[-1:]))
        if level == LEVELS - 1:
            v = v + w * r
            r = resid(v, source, s, earlier(v[-1:]))
        masked = jnp.where(own[None, :, None], r, 0.0)
        norms.append((masked * masked).reshape(-1, 8, 128).sum(0))
        sources.append(source)
        fields.append(v)
        if level < LEVELS - 1:
            source = r[0::2] + r[1::2]
    field = fields[-1]
    for level in range(LEVELS - 2, 0, -1):
        s = 2.0**level * s_win
        w = DAMPING / (1.0 + 4.0 * s)
        field = fields[level - 1] + jnp.repeat(field, 2, axis=0)
        field = field + w * resid(field, sources[level - 1], s, earlier(field[-1:]))
    past = jnp.concatenate([earlier(field[-1:]), field[:-1]], axis=0)
    field, past = [x[:, REACH : x.shape[1] - REACH] for x in (field, past)]
    half = -(-field.shape[1] // 2)
    even = jnp.concatenate([past, field[:, :half]], axis=1)
    odd = jnp.concatenate([field, past[:, -half:]], axis=1)
    both = jnp.where((jnp.arange(TEAM) % 2 == 1)[:, None, None], odd, even)
    return both.reshape(*both.shape[:2], 8, 128), jnp.stack(norms)


def body(count, strips, rhs, guess, diffusion):
    points, rows, cells = rhs.shape
    assert points == 2 and cells == 1024 and count % TEAM == 0
    assert rows % (8 * TEAM) == 0
    total_cells = rows * strips * cells
    groups = rows // 8
    piece, window, start_of = windows_of(rows)
    half_piece = -(-piece // 2)
    wide = cells // 16
    ext = rows + 2 * HALO

    def both(first):
        pairs = [(i, i + 1) for i in range(first, strips - 1, 2)]
        return pairs + [(b, a) for a, b in pairs]

    later = [(i, i + 1) for i in range(count - 1)]

    rhs_t, guess_t, diff_t = tiles(rhs), tiles(guess), tiles(diffusion)
    edge_groups = -(-HALO // 8)
    assert groups % edge_groups == 0
    far = groups // edge_groups - 1

    def edge_specs(block):
        time = pl.BlockSpec((2, edge_groups, wide, 128), lambda i: (0, block, 0, 0))
        flat = pl.BlockSpec((edge_groups, wide, 128), lambda i: (block, 0, 0))
        return [time, time, flat]

    far_args = [pltpu.with_memory_space_constraint(x, pltpu.HBM) for x in (guess_t, rhs_t, diff_t)]
    (g_prev,) = kernel_call(
        take_later,
        [shape(groups, wide, 128)],
        specs=[pl.BlockSpec(memory_space=pl.ANY)],
        more=[pltpu.SemaphoreType.DMA(())] * 4,
    )(far_args[0])
    g_prev = lax.ppermute(g_prev, "tm", later)
    facing, backing = kernel_call(
        pack_edges, [shape(5 * HALO, 8, 128)] * 2, specs=edge_specs(0) + edge_specs(far), grid=(1,)
    )(*far_args, *far_args)
    facing = lax.ppermute(facing, "space", both(0))
    backing = lax.ppermute(backing, "space", both(1))
    (send,) = kernel_call(first_sweep, [shape(rows, 8, 128)], scratch=[(rows + 2, 8, 128)], n_in=3)(
        guess_t, rhs_t, diff_t
    )
    got = lax.ppermute(send, "tm", later)
    s_ext, w_ext, part0, left0, left1, v1, edges = kernel_call(
        local_parts,
        [kept(ext, 8, 128)] * 2 + [shape(ext, 8, 128)] * 4 + [shape(4 * SIDE, 8, 128)],
        scratch=[(ext, 8, 128)] * 2 + [(5 * HALO, 8, 128)] * 2,
        n_in=5,
    )(guess_t, rhs_t, diff_t, facing, backing)
    edges = lax.ppermute(edges, "tm", later)
    *mine, y, resid0 = kernel_call(
        functools.partial(join_first, start_of, window),
        [shape(window, 8, 128)] * TEAM + [shape(ext, 8, 128)] * 2,
        scratch=[(ext, 8, 128)],
        n_in=7,
    )(g_prev, got, edges, s_ext, w_ext, left0, left1)

    def exchange(order, parts):
        moved = list(parts)
        for k in order:
            moved[k] = lax.ppermute(parts[k], "tm", [(i, i ^ k) for i in range(count)])
        return moved

    mine = exchange(DOWN, mine)
    base0, base1, back, norm0 = kernel_call(
        join_rest,
        [kept(rows + 2, 8, 128)] * 2 + [shape(rows, 8, 128), shape(8, 128)],
        n_in=6,
    )(w_ext, part0, left1, v1, y, resid0)
    back = lax.ppermute(back, "tm", later)
    if count == TEAM:
        tall = padded(window)
        half = [(TEAM >> level, tall, 8, 128) for level in range(LEVELS)]
        bases = []
        for level in range(1, LEVELS - 1):
            bases += [half[level - 1], half[level]]
        *fields, norms = kernel_call(
            functools.partial(coarse_levels, start_of, rows),
            [shape(piece + half_piece, 8, 128)] * TEAM + [shape(LEVELS - 1, 8, 128)],
            scratch=[(tall, 8, 128), (LEVELS - 1, tall, 8, 128), half[0], half[0], (TEAM + 1, piece, 8, 128)] + bases,
            n_in=1 + TEAM,
        )(s_ext, *mine)
    else:
        place = place_of()
        order = place ^ jnp.arange(TEAM)
        start = start_of(place) - REACH
        s_win = lax.dynamic_slice_in_dim(s_ext, start + HALO, window, axis=0)
        at = start + jnp.arange(window) - place * (rows // TEAM)
        own = (at >= 0) & (at < rows // TEAM)
        jumps = [(i, i + TEAM) for i in range(count - TEAM)]
        fields, norms = coarse_plain(jnp.stack(mine)[order], s_win, own, lambda v: lax.ppermute(v, "tm", jumps))
        fields = list(fields[order])
    fields = exchange(UP, fields)

    s_ext, w_ext, base0, base1 = keep(s_ext, w_ext, base0, base1)
    (halves,) = kernel_call(
        functools.partial(pick_halves, piece), [shape(TEAM * half_piece, 8, 128)], n_in=TEAM
    )(*fields)
    halves = lax.ppermute(halves, "tm", [(i, i ^ 1) for i in range(count)])
    own, own_spread = kernel_call(
        functools.partial(spread_own, start_of, piece),
        [shape(rows + 2 * EDGE, 8, 128), shape(rows + 2, 8, 128)],
        n_in=2 + TEAM,
    )(s_ext, w_ext, *fields)
    out, left, norm = kernel_call(
        functools.partial(finish, start_of, piece),
        [shape(2, groups, wide, 128), shape(rows, 8, 128), shape(8, 128)],
        scratch=[(rows + 2 * EDGE, 8, 128)] + [(rows + 2, 8, 128)] * 3 + [(2, groups, wide, 128)],
        more=[pltpu.SemaphoreType.DMA(())] * 4,
        out_specs=[pl.BlockSpec(memory_space=pl.ANY), vmem(), vmem()],
        n_in=8 + TEAM,
    )(rhs_t, s_ext, w_ext, base0, base1, own, own_spread, halves, *fields)
    (sums,) = kernel_call(add_up, [shape(8, 128)], n_in=5)(left, back, norm0, norms, norm)

    every = jnp.broadcast_to(sums[None], (count * strips, 8, 128))
    every = lax.all_to_all(every, ("tm", "space"), 0, 0)
    totals = every.sum(axis=(0, 2))[: LEVELS + 1]
    return untiles(out), jnp.sqrt(totals / total_cells)


def solution(mesh):
    in_specs = (P("tm", "space", None), P("tm", "space", None), P("space", None))
    out_specs = (P("tm", "space", None), P())
    step = functools.partial(body, mesh.shape["tm"], mesh.shape["space"])
    step = jax.shard_map(step, mesh=mesh, in_specs=in_specs, out_specs=out_specs, check_vma=False)
    return step
```

```python
import functools
import math
import jax
import jax.numpy as jnp
from jax import lax
from jax.experimental import pallas as pl
from jax.experimental.pallas import tpu as pltpu
from jax.sharding import PartitionSpec as P

LEVELS = 5
DAMPING = 0.8
KEEP = 1.0 - DAMPING
GROUP = 2 ** (LEVELS - 1)
TEAM = GROUP // 2
DOWN = (2, 6, 4, 3, 7, 5, 1)
UP = (2, 6, 4, 3, 7, 5, 1)
HALO = 2 * LEVELS + 1
SIDE = HALO - 1
EDGE = 2
REACH = 2 * LEVELS - 3


def vmem():
    return pl.BlockSpec(memory_space=pltpu.VMEM)


def shape(*dims):
    return jax.ShapeDtypeStruct(dims, jnp.float32)


def kept(*dims):
    return pltpu.VMEM(dims, jnp.float32)


def keep(*arrays):
    return [pltpu.with_memory_space_constraint(x, pltpu.VMEM) for x in arrays]


def kernel_call(body, outs, scratch=(), flops=0, n_in=0, specs=None, grid=(), more=(), out_specs=None):
    def call(*args):
        held = sum(math.prod(dims) for dims in scratch)
        held += sum(math.prod(x.shape) for x in list(outs) + list(args))
        return pl.pallas_call(
            body,
            out_shape=outs,
            grid=grid,
            in_specs=specs or [vmem() for _ in range(n_in)],
            out_specs=out_specs or [vmem() for _ in outs],
            scratch_shapes=[pltpu.VMEM(dims, jnp.float32) for dims in scratch] + list(more),
            compiler_params=pltpu.CompilerParams(vmem_limit_bytes=4 * held + 2**21),
            cost_estimate=pl.CostEstimate(flops=flops, bytes_accessed=flops, transcendentals=0),
        )(*args)

    return call


def tiles(block):
    lead = block.shape[:-2]
    rows, cells = block.shape[-2:]
    split = block.reshape(*lead, rows // 8, 8, cells // 128, 128)
    return jnp.swapaxes(split, -3, -2).reshape(*lead, rows // 8, cells // 16, 128)


def untiles(block):
    lead = block.shape[:-3]
    groups, wide, _ = block.shape[-3:]
    split = block.reshape(*lead, groups, wide // 8, 8, 128)
    return jnp.swapaxes(split, -3, -2).reshape(*lead, groups * 8, wide * 16)


def masks():
    sub = lax.broadcasted_iota(jnp.int32, (8, 128), 0)
    lane = lax.broadcasted_iota(jnp.int32, (8, 128), 1)
    first = lane == 0
    last = lane == 127
    return first, last, first & (sub == 0), last & (sub == 7)


def beside(row, m):
    first, last, left_end, right_end = m
    left = pltpu.roll(row, 1, 1)
    left = jnp.where(first, pltpu.roll(left, 1, 0), left)
    right = pltpu.roll(row, 127, 1)
    right = jnp.where(last, pltpu.roll(right, 7, 0), right)
    return jnp.where(left_end, 0.0, left) + jnp.where(right_end, 0.0, right)


def around(ref, row, m):
    return beside(ref[row], m) + (ref[row - 1] + ref[row + 1])


def loop(low, high, body, carry=None, unroll=4):
    quiet = carry is None
    steps = (high - low) // unroll

    def block(n, value):
        for k in range(unroll):
            value = (body(low + n * unroll + k), value)[1] if quiet else body(low + n * unroll + k, value)
        return value

    value = lax.fori_loop(0, steps, block, 0 if quiet else carry)
    for i in range(low + steps * unroll, high):
        value = (body(i), value)[1] if quiet else body(i, value)
    return None if quiet else value


BLOCK = 64


def padded(rows):
    return -(-(rows - 2) // BLOCK) * BLOCK + 2


def block_loop(low, high, body, carry, unroll):
    high = low + -(-(high - low) // unroll) * unroll
    return loop(low, high, body, carry, unroll)


def strided(ref, lead, row_group, k):
    return ref[lead + (row_group, pl.ds(k, 8, stride=8))]


def place_of():
    return lax.rem(lax.axis_index("tm"), TEAM)


def odd_strip():
    return lax.rem(lax.axis_index("space"), 2) == 1


def either(flag, body, one, two):
    pl.when(flag)(lambda: body(two, one))
    pl.when(jnp.logical_not(flag))(lambda: body(one, two))


def take_later(guess, out, *done):
    part = out.shape[0] // len(done)
    copies = []
    for k, sem in enumerate(done):
        at = pl.ds(k * part, part)
        copies.append(pltpu.make_async_copy(guess.at[1, at], out.at[at], sem))
    for copy in copies:
        copy.start()
    for copy in copies:
        copy.wait()


def pack_edges(g_top, r_top, d_top, g_end, r_end, d_end, pair, other):
    count = g_top.shape[1] * 8
    refs = [((g_top, (t,)), (g_end, (t,))) for t in range(2)]
    refs += [((r_top, (t,)), (r_end, (t,))) for t in range(2)]
    refs += [((d_top, ()), (d_end, ()))]

    def fill(end, top):
        for i, ((a, lead_a), (b, lead_b)) in enumerate(refs):
            for k in range(HALO):
                top[i * HALO + k] = strided(a, lead_a, k // 8, k % 8)
                row = count - HALO + k
                end[i * HALO + k] = strided(b, lead_b, row // 8, row % 8)

    either(odd_strip(), fill, pair, other)


def first_sweep(guess, rhs, diff, send, g1):
    rows = guess.shape[1] * 8
    m = masks()

    def unpack(g):
        for k in range(8):
            i = g * 8 + k
            g1[1 + i] = strided(guess, (1,), g, k)

    loop(0, rows // 8, unpack, unroll=2)

    def sweep(g):
        for k in range(8):
            i = g * 8 + k
            s = strided(diff, (), g, k)
            w = DAMPING / (1.0 + 4.0 * s)
            whole = strided(rhs, (1,), g, k) + s * around(g1, 1 + i, m) + strided(guess, (0,), g, k)
            send[i] = KEEP * g1[1 + i] + w * whole

    loop(0, rows // 8, sweep, unroll=4)


def local_parts(guess, rhs, diff, pair, other, s_ext, w_ext, part0, left0, left1, v1, edges, g0, g1, low, high, drift):
    rows = rhs.shape[1] * 8
    m = masks()

    def unpack(g):
        for k in range(8):
            i = HALO + g * 8 + k
            s = strided(diff, (), g, k)
            s_ext[i] = s
            w_ext[i] = DAMPING / (1.0 + 4.0 * s)
            g0[i] = strided(guess, (0,), g, k)
            g1[i] = strided(guess, (1,), g, k)

    def order(after, before):
        for k in range(5 * HALO):
            low[k] = before[k]
            high[k] = after[k]

    either(odd_strip(), order, pair, other)
    loop(0, rows // 8, unpack, unroll=2)
    for k in range(HALO):
        for dst, i in ((g0, 0), (g1, 1), (s_ext, 4)):
            dst[k] = low[i * HALO + k]
            dst[HALO + rows + k] = high[i * HALO + k]
        for i in (k, HALO + rows + k):
            w_ext[i] = DAMPING / (1.0 + 4.0 * s_ext[i])

    def fill(i, a, b):
        s = s_ext[i]
        w = w_ext[i]
        part0[i] = KEEP * g0[i] + w * (a + s * around(g0, i, m))
        v1[i] = KEEP * g1[i] + w * (b + s * around(g1, i, m) + g0[i])

    def inner(g):
        for k in range(8):
            fill(HALO + g * 8 + k, strided(rhs, (0,), g, k), strided(rhs, (1,), g, k))

    loop(0, rows // 8, inner, unroll=2)
    for k in range(1, HALO):
        fill(k, low[2 * HALO + k], low[3 * HALO + k])
    for k in range(0, HALO - 1):
        fill(HALO + rows + k, high[2 * HALO + k], high[3 * HALO + k])
    ends = [(2, HALO - 1), (HALO + rows, 2 * HALO + rows - 3)]
    for n, (first, final) in enumerate(ends):
        for i in range(first - 1, final + 2):
            drift[n * (SIDE + 1) + i - first + 1] = w_ext[i] * g1[i]
    for n, (first, final) in enumerate(ends):
        for i in range(first, final + 1):
            at = n * (SIDE + 1) + i - first + 1
            s = s_ext[i]
            here = drift[at]
            edges[n * (SIDE - 1) + i - first] = v1[i] - 4.0 * s * here + s * around(drift, at, m)
    low_at = 2 * (SIDE - 1)
    edges[low_at] = w_ext[HALO - 1] * g1[HALO - 1]
    edges[low_at + 1] = w_ext[HALO + rows] * g1[HALO + rows]
    edges[low_at + 2] = v1[HALO]
    edges[low_at + 3] = v1[HALO + rows - 1]

    def rest(i, a, b):
        s = s_ext[i]
        diag = 1.0 + 4.0 * s
        left0[i] = a - diag * part0[i] + s * around(part0, i, m)
        left1[i] = b - diag * v1[i] + s * around(v1, i, m) + part0[i]

    def inner2(g):
        for k in range(8):
            rest(HALO + g * 8 + k, strided(rhs, (0,), g, k), strided(rhs, (1,), g, k))

    loop(0, rows // 8, inner2, unroll=2)
    for k in range(2, HALO):
        rest(k, low[2 * HALO + k], low[3 * HALO + k])
    for k in range(0, HALO - 2):
        rest(HALO + rows + k, high[2 * HALO + k], high[3 * HALO + k])


def windows_of(rows):
    piece = -(-(rows + 2 * EDGE) // TEAM)
    spare = rows + 2 * EDGE - piece

    def start(j):
        return j * spare // (TEAM - 1) - EDGE

    return piece, piece + 2 * REACH, start


def join_first(start_of, window, g_prev, got, edges, s_ext, w_ext, left0, left1, *refs):
    outs = refs[:TEAM]
    y, resid0, coarse = refs[TEAM:]
    place = place_of()
    rows = got.shape[0]
    m = masks()

    def inner(g):
        for k in range(8):
            i = HALO + g * 8 + k
            y[i] = w_ext[i] * strided(g_prev, (), g, k)

    loop(0, rows // 8, inner, unroll=2)
    single = 2 * (SIDE - 1)
    y[HALO - 1] = edges[single]
    y[HALO + rows] = edges[single + 1]

    def resid(i, swept):
        s = s_ext[i]
        here = y[i]
        a = left0[i] - (1.0 + 4.0 * s) * here + s * around(y, i, m) + swept
        resid0[i] = a
        coarse[i] = a + left1[i] + here

    loop(HALO + 1, HALO + rows - 1, lambda i: resid(i, got[i - HALO]), unroll=32)
    resid(HALO, edges[single + 2])
    resid(HALO + rows - 1, edges[single + 3])
    for k in range(SIDE - 1):
        for i, at in ((2 + k, k), (HALO + rows + k, SIDE - 1 + k)):
            taken = left0[i] + edges[at]
            coarse[i] = taken + left1[i]
            if i in (HALO - 1, HALO + rows):
                resid0[i] = taken - y[i]
    for k, out in enumerate(outs):
        low = start_of(place ^ k) - REACH + HALO

        def copy(i, out=out, low=low):
            out[i] = coarse[low + i]

        loop(0, window, copy, unroll=16)


def join_rest(w_ext, part0, left1, v1, y, resid0, base0, base1, back, norm):
    rows = back.shape[0]

    def based(i):
        w = w_ext[i]
        a = resid0[i]
        b = left1[i] + y[i]
        base0[i - HALO + 1] = part0[i] + y[i] + w * a
        value = v1[i] + w * b
        base1[i - HALO + 1] = value
        return a, b, value

    def main(i, acc):
        a, b, value = based(i)
        back[i - HALO] = value
        return acc + (a * a + b * b)

    norm[...] = loop(HALO, HALO + rows, main, jnp.zeros((8, 128), jnp.float32), unroll=8)
    based(HALO - 1)
    based(HALO + rows)


def coarse_levels(start_of, rows, s_ext, *refs):
    g_in, refs = refs[:TEAM], refs[TEAM:]
    outs, refs = refs[:TEAM], refs[TEAM:]
    norms, s_win, w_win, v_ref, e_ref, final = refs[:6]
    bases = refs[6:]
    window = g_in[0].shape[0]
    piece = window - 2 * REACH
    m = masks()
    place = place_of()
    start = start_of(place) - REACH
    first_own = place * (rows // TEAM) - start
    last_own = first_own + rows // TEAM

    def level_weights(i):
        s = s_ext[start + HALO + i]
        s_win[i] = s
        for level in range(1, LEVELS):
            w_win[level - 1, i] = DAMPING / (1.0 + 4.0 * 2.0**level * s)

    loop(0, window, level_weights, unroll=4)

    def own(i, value):
        return jnp.where((i >= first_own) & (i < last_own), value, 0.0)

    source = None
    zero = jnp.zeros((8, 128), jnp.float32)
    for level in range(1, LEVELS - 1):
        points = TEAM >> (level - 1)
        lost = level - 1
        base = bases[2 * (level - 1)]
        target = bases[2 * (level - 1) + 1]

        def smooth(i, level=level, points=points, source=source):
            w = w_win[level - 1, i]
            for p in range(points):
                if source is None:
                    v_ref[place ^ p, i] = w * g_in[p][i]
                else:
                    v_ref[p, i] = w * source[p, i]

        loop(0, window, smooth, unroll=4)

        def descend(i, acc, level=level, points=points, source=source, base=base, target=target):
            s = 2.0**level * s_win[i]
            w = w_win[level - 1, i]
            pairs = []
            total = zero
            before = None
            for p in range(points):
                here = v_ref[p, i]
                r = 0.25 * here + s * (here + beside(here, m) + (v_ref[p, i - 1] + v_ref[p, i + 1]))
                if before is not None:
                    r = r + before
                base[p, i] = here + w * r
                total = total + r * r
                pairs.append(r)
                before = here
            for q in range(points // 2):
                target[q, i] = pairs[2 * q] + pairs[2 * q + 1]
            return acc + own(i, total)

        norms[level - 1] = block_loop(1, window - 1, descend, zero, BLOCK // points)
        source = target

    level = LEVELS - 1
    lost = level - 1

    def smooth_last(i):
        v_ref[0, i] = w_win[level - 1, i] * source[0, i]

    loop(0, window, smooth_last, unroll=16)

    def again(i):
        s = 2.0**level * s_win[i]
        here = v_ref[0, i]
        r = 0.25 * here + s * (here + beside(here, m) + (v_ref[0, i - 1] + v_ref[0, i + 1]))
        e_ref[0, i] = here + w_win[level - 1, i] * r

    block_loop(1, window - 1, again, None, BLOCK)

    def last_residual(i, acc):
        s = 2.0**level * s_win[i]
        here = e_ref[0, i]
        r = source[0, i] - (1.0 + 4.0 * s) * here
        r = r + s * (beside(here, m) + (e_ref[0, i - 1] + e_ref[0, i + 1]))
        return acc + own(i, r * r)

    norms[level - 1] = block_loop(1, window - 1, last_residual, zero, BLOCK)

    lost = LEVELS - 1
    field, other = e_ref, v_ref
    for level in range(LEVELS - 2, 0, -1):
        points = TEAM >> (level - 1)
        lost += 1
        base = bases[2 * (level - 1)]

        def ascend(i, level=level, points=points, base=base, field=field, other=other):
            s = 2.0**level * s_win[i]
            w = w_win[level - 1, i]
            before = None
            for q in range(points // 2):
                e = field[q, i]
                part = KEEP * e + w * (s * (beside(e, m) + (field[q, i - 1] + field[q, i + 1])))
                kept = w * e
                for p in (2 * q, 2 * q + 1):
                    value = base[p, i] + part
                    drift = before if p == 2 * q else kept
                    if drift is not None:
                        value = value + drift
                    if level == 1:
                        final[p + 1, i - REACH] = value
                    else:
                        other[p, i] = value
                before = kept

        span = BLOCK // points * 2
        if level == 1:
            loop(lost, window - lost, ascend, unroll=11)
        else:
            block_loop(1, window - 1, ascend, None, span)
        field, other = other, field

    def blank(i):
        final[0, i] = zero

    loop(0, piece, blank, unroll=11)
    for k, out in enumerate(outs):

        target = place ^ k
        odd = lax.rem(target, 2)
        half = out.shape[0] - piece

        def copy(i, out=out, at=target + odd):
            out[i] = final[at, i]

        def copy_half(i, out=out, at=target - odd + 1, skip=odd * (piece - half), half=half):
            out[piece + i] = final[at, skip + i]

        loop(0, piece, copy, unroll=11)
        loop(0, half, copy_half, unroll=17)


def odd_place():
    return lax.rem(lax.axis_index("tm"), 2)


def pick_halves(piece, *refs):
    fields, (out,) = refs[:TEAM], refs[TEAM:]
    half = fields[0].shape[0] - piece
    place = place_of()
    for k, got in enumerate(fields):
        first = (place ^ k) * half

        def copy(i, got=got, first=first):
            out[first + i] = got[piece + i]

        loop(0, half, copy, unroll=17)


def spread(field, s_ext, w_ext, out):
    m = masks()

    def body(i):
        s = s_ext[i + HALO - 1]
        out[i] = KEEP * field[i + 1] + w_ext[i + HALO - 1] * (s * around(field, i + 1, m))

    loop(0, out.shape[0], body, unroll=43)


def spread_own(start_of, piece, s_ext, w_ext, *refs):
    fields, (own, out) = refs[:TEAM], refs[TEAM:]
    place = place_of()
    for k, got in enumerate(fields):
        start = start_of(place ^ k) + EDGE

        def copy(i, got=got, start=start):
            own[start + i] = got[i]

        loop(0, piece, copy, unroll=11)
    spread(own, s_ext, w_ext, out)


def finish(start_of, piece, rhs, s_ext, w_ext, base0, base1, own, own_spread, halves, *refs):
    fields = refs[:TEAM]
    whole, left, norm, shared, shared_spread, sol0, sol1, out, *done = refs[TEAM:]
    groups = rhs.shape[1]
    share = groups // len(done)
    rows = rhs.shape[1] * 8
    half = fields[0].shape[0] - piece
    m = masks()
    place = place_of()
    odd = odd_place()
    skip = odd * (piece - half)
    for k, got in enumerate(fields):
        start = start_of(place ^ k) + EDGE + skip

        def copy(i, got=got, start=start):
            shared[start + i] = got[piece + i]

        loop(0, half, copy, unroll=17)
    for j in range(TEAM):
        start = start_of(j) + EDGE + (piece - half) - skip

        def copy(i, j=j, start=start):
            shared[start + i] = halves[j * half + i]

        loop(0, half, copy, unroll=17)
    spread(shared, s_ext, w_ext, shared_spread)

    def solve(now, before):
        e, part = now
        past, past_part = before

        def correct(i):
            w = w_ext[i + HALO - 1]
            sol0[i] = base0[i] + part[i] + w * past[i + 1]
            sol1[i] = base1[i] + part[i] + w * e[i + 1]

        loop(0, rows + 2, correct, unroll=16)

        def last(g, acc):
            for k in range(8):
                i = g * 8 + k
                s = s_ext[i + HALO]
                diag = 1.0 + 4.0 * s
                older = past_part[i + 1] + w_ext[i + HALO] * past[i + EDGE]
                a = sol0[i + 1]
                b = sol1[i + 1]
                left[i] = strided(rhs, (0,), g, k) - diag * a + s * around(sol0, i + 1, m) + older
                rb = strided(rhs, (1,), g, k) - diag * b + s * around(sol1, i + 1, m) + a
                out[0, g, pl.ds(k, 8, stride=8)] = a
                out[1, g, pl.ds(k, 8, stride=8)] = b
                acc = acc + rb * rb
            return acc

        acc = jnp.zeros((8, 128), jnp.float32)
        copies = []
        for n, sem in enumerate(done):
            acc = loop(n * share, (n + 1) * share, last, acc, unroll=4)
            at = pl.ds(n * share, share)
            copies.append(pltpu.make_async_copy(out.at[:, at], whole.at[:, at], sem))
            copies[-1].start()
        norm[...] = acc
        for copy in copies:
            copy.wait()

    either(odd == 1, solve, (shared, shared_spread), (own, own_spread))


def add_up(left, back, norm0, norms, norm, sums):
    def body(i, acc):
        r = left[i] + back[i]
        return acc + r * r

    acc = loop(0, back.shape[0], body, norm[...], unroll=16)
    parts = [norm0[...]] + [norms[k] for k in range(LEVELS - 1)] + [acc]
    for k, part in enumerate(parts):
        sums[pl.ds(k, 1)] = jnp.sum(part, axis=0, keepdims=True)
    for k in range(len(parts), 8):
        sums[pl.ds(k, 1)] = jnp.zeros((1, 128), jnp.float32)


def coarse_plain(g_in, s_win, own, earlier):
    cells = g_in.shape[-2] * 128

    def flat(x):
        return x.reshape(*x.shape[:-2], cells)

    def around_plain(v):
        padded = jnp.pad(v, ((0, 0), (1, 1), (1, 1)))
        total = padded[:, 2:, 1:-1] + padded[:, :-2, 1:-1]
        return total + padded[:, 1:-1, 2:] + padded[:, 1:-1, :-2]

    def resid(v, g, s, before):
        past = jnp.concatenate([before, v[:-1]], axis=0)
        return g - (1.0 + 4.0 * s) * v + s * around_plain(v) + past

    source = flat(g_in)
    s_win = flat(s_win)
    sources, fields, norms = [], [], []
    for level in range(1, LEVELS):
        s = 2.0**level * s_win
        w = DAMPING / (1.0 + 4.0 * s)
        v = w * source
        r = resid(v, source, s, earlier(v[-1:]))
        if level == LEVELS - 1:
            v = v + w * r
            r = resid(v, source, s, earlier(v[-1:]))
        masked = jnp.where(own[None, :, None], r, 0.0)
        norms.append((masked * masked).reshape(-1, 8, 128).sum(0))
        sources.append(source)
        fields.append(v)
        if level < LEVELS - 1:
            source = r[0::2] + r[1::2]
    field = fields[-1]
    for level in range(LEVELS - 2, 0, -1):
        s = 2.0**level * s_win
        w = DAMPING / (1.0 + 4.0 * s)
        field = fields[level - 1] + jnp.repeat(field, 2, axis=0)
        field = field + w * resid(field, sources[level - 1], s, earlier(field[-1:]))
    past = jnp.concatenate([earlier(field[-1:]), field[:-1]], axis=0)
    field, past = [x[:, REACH : x.shape[1] - REACH] for x in (field, past)]
    half = -(-field.shape[1] // 2)
    even = jnp.concatenate([past, field[:, :half]], axis=1)
    odd = jnp.concatenate([field, past[:, -half:]], axis=1)
    both = jnp.where((jnp.arange(TEAM) % 2 == 1)[:, None, None], odd, even)
    return both.reshape(*both.shape[:2], 8, 128), jnp.stack(norms)


def body(count, strips, rhs, guess, diffusion):
    points, rows, cells = rhs.shape
    assert points == 2 and cells == 1024 and count % TEAM == 0
    assert rows % (8 * TEAM) == 0
    total_cells = rows * strips * cells
    groups = rows // 8
    piece, window, start_of = windows_of(rows)
    half_piece = -(-piece // 2)
    wide = cells // 16
    ext = rows + 2 * HALO

    def both(first):
        pairs = [(i, i + 1) for i in range(first, strips - 1, 2)]
        return pairs + [(b, a) for a, b in pairs]

    later = [(i, i + 1) for i in range(count - 1)]

    rhs_t, guess_t, diff_t = tiles(rhs), tiles(guess), tiles(diffusion)
    edge_groups = -(-HALO // 8)
    assert groups % edge_groups == 0
    far = groups // edge_groups - 1

    def edge_specs(block):
        time = pl.BlockSpec((2, edge_groups, wide, 128), lambda i: (0, block, 0, 0))
        flat = pl.BlockSpec((edge_groups, wide, 128), lambda i: (block, 0, 0))
        return [time, time, flat]

    far_args = [pltpu.with_memory_space_constraint(x, pltpu.HBM) for x in (guess_t, rhs_t, diff_t)]
    (g_prev,) = kernel_call(
        take_later,
        [shape(groups, wide, 128)],
        specs=[pl.BlockSpec(memory_space=pl.ANY)],
        more=[pltpu.SemaphoreType.DMA(())] * 4,
    )(far_args[0])
    g_prev = lax.ppermute(g_prev, "tm", later)
    facing, backing = kernel_call(
        pack_edges, [shape(5 * HALO, 8, 128)] * 2, specs=edge_specs(0) + edge_specs(far), grid=(1,)
    )(*far_args, *far_args)
    facing = lax.ppermute(facing, "space", both(0))
    backing = lax.ppermute(backing, "space", both(1))
    (send,) = kernel_call(first_sweep, [shape(rows, 8, 128)], scratch=[(rows + 2, 8, 128)], n_in=3)(
        guess_t, rhs_t, diff_t
    )
    got = lax.ppermute(send, "tm", later)
    s_ext, w_ext, part0, left0, left1, v1, edges = kernel_call(
        local_parts,
        [kept(ext, 8, 128)] * 2 + [shape(ext, 8, 128)] * 4 + [shape(2 * SIDE + 2, 8, 128)],
        scratch=[(ext, 8, 128)] * 2 + [(5 * HALO, 8, 128)] * 2 + [(2 * (SIDE + 1), 8, 128)],
        n_in=5,
    )(guess_t, rhs_t, diff_t, facing, backing)
    edges = lax.ppermute(edges, "tm", later)
    *mine, y, resid0 = kernel_call(
        functools.partial(join_first, start_of, window),
        [shape(window, 8, 128)] * TEAM + [shape(ext, 8, 128)] * 2,
        scratch=[(ext, 8, 128)],
        n_in=7,
    )(g_prev, got, edges, s_ext, w_ext, left0, left1)

    def exchange(order, parts):
        moved = list(parts)
        for k in order:
            moved[k] = lax.ppermute(parts[k], "tm", [(i, i ^ k) for i in range(count)])
        return moved

    mine = exchange(DOWN, mine)
    base0, base1, back, norm0 = kernel_call(
        join_rest,
        [kept(rows + 2, 8, 128)] * 2 + [shape(rows, 8, 128), shape(8, 128)],
        n_in=6,
    )(w_ext, part0, left1, v1, y, resid0)
    back = lax.ppermute(back, "tm", later)
    if count == TEAM:
        tall = padded(window)
        half = [(TEAM >> level, tall, 8, 128) for level in range(LEVELS)]
        bases = []
        for level in range(1, LEVELS - 1):
            bases += [half[level - 1], half[level]]
        *fields, norms = kernel_call(
            functools.partial(coarse_levels, start_of, rows),
            [shape(piece + half_piece, 8, 128)] * TEAM + [shape(LEVELS - 1, 8, 128)],
            scratch=[(tall, 8, 128), (LEVELS - 1, tall, 8, 128), half[0], half[0], (TEAM + 1, piece, 8, 128)] + bases,
            n_in=1 + TEAM,
        )(s_ext, *mine)
    else:
        place = place_of()
        order = place ^ jnp.arange(TEAM)
        start = start_of(place) - REACH
        s_win = lax.dynamic_slice_in_dim(s_ext, start + HALO, window, axis=0)
        at = start + jnp.arange(window) - place * (rows // TEAM)
        own = (at >= 0) & (at < rows // TEAM)
        jumps = [(i, i + TEAM) for i in range(count - TEAM)]
        fields, norms = coarse_plain(jnp.stack(mine)[order], s_win, own, lambda v: lax.ppermute(v, "tm", jumps))
        fields = list(fields[order])
    fields = exchange(UP, fields)

    s_ext, w_ext, base0, base1 = keep(s_ext, w_ext, base0, base1)
    (halves,) = kernel_call(
        functools.partial(pick_halves, piece), [shape(TEAM * half_piece, 8, 128)], n_in=TEAM
    )(*fields)
    halves = lax.ppermute(halves, "tm", [(i, i ^ 1) for i in range(count)])
    own, own_spread = kernel_call(
        functools.partial(spread_own, start_of, piece),
        [shape(rows + 2 * EDGE, 8, 128), shape(rows + 2, 8, 128)],
        n_in=2 + TEAM,
    )(s_ext, w_ext, *fields)
    out, left, norm = kernel_call(
        functools.partial(finish, start_of, piece),
        [shape(2, groups, wide, 128), shape(rows, 8, 128), shape(8, 128)],
        scratch=[(rows + 2 * EDGE, 8, 128)] + [(rows + 2, 8, 128)] * 3 + [(2, groups, wide, 128)],
        more=[pltpu.SemaphoreType.DMA(())] * 4,
        out_specs=[pl.BlockSpec(memory_space=pl.ANY), vmem(), vmem()],
        n_in=8 + TEAM,
    )(rhs_t, s_ext, w_ext, base0, base1, own, own_spread, halves, *fields)
    (sums,) = kernel_call(add_up, [shape(8, 128)], n_in=5)(left, back, norm0, norms, norm)

    every = jnp.broadcast_to(sums[None], (count * strips, 8, 128))
    every = lax.all_to_all(every, ("tm", "space"), 0, 0)
    totals = every.sum(axis=(0, 2))[: LEVELS + 1]
    return untiles(out), jnp.sqrt(totals / total_cells)


def solution(mesh):
    in_specs = (P("tm", "space", None), P("tm", "space", None), P("space", None))
    out_specs = (P("tm", "space", None), P())
    step = functools.partial(body, mesh.shape["tm"], mesh.shape["space"])
    step = jax.shard_map(step, mesh=mesh, in_specs=in_specs, out_specs=out_specs, check_vma=False)
    return step
```

```python
import functools
import math
import jax
import jax.numpy as jnp
from jax import lax
from jax.experimental import pallas as pl
from jax.experimental.pallas import tpu as pltpu
from jax.sharding import PartitionSpec as P

LEVELS = 5
DAMPING = 0.8
KEEP = 1.0 - DAMPING
GROUP = 2 ** (LEVELS - 1)
TEAM = GROUP // 2
DOWN = (2, 6, 4, 3, 7, 5, 1)
UP = (2, 6, 4, 3, 7, 5, 1)
HALO = 2 * LEVELS + 1
SIDE = HALO - 1
EDGE = 2
REACH = 2 * LEVELS - 3


def vmem():
    return pl.BlockSpec(memory_space=pltpu.VMEM)


def shape(*dims):
    return jax.ShapeDtypeStruct(dims, jnp.float32)


def kept(*dims):
    return pltpu.VMEM(dims, jnp.float32)


def keep(*arrays):
    return [pltpu.with_memory_space_constraint(x, pltpu.VMEM) for x in arrays]


def kernel_call(body, outs, scratch=(), flops=0, n_in=0, specs=None, grid=(), more=(), out_specs=None):
    def call(*args):
        held = sum(math.prod(dims) for dims in scratch)
        held += sum(math.prod(x.shape) for x in list(outs) + list(args))
        return pl.pallas_call(
            body,
            out_shape=outs,
            grid=grid,
            in_specs=specs or [vmem() for _ in range(n_in)],
            out_specs=out_specs or [vmem() for _ in outs],
            scratch_shapes=[pltpu.VMEM(dims, jnp.float32) for dims in scratch] + list(more),
            compiler_params=pltpu.CompilerParams(vmem_limit_bytes=4 * held + 2**21),
            cost_estimate=pl.CostEstimate(flops=flops, bytes_accessed=flops, transcendentals=0),
        )(*args)

    return call


def tiles(block):
    lead = block.shape[:-2]
    rows, cells = block.shape[-2:]
    split = block.reshape(*lead, rows // 8, 8, cells // 128, 128)
    return jnp.swapaxes(split, -3, -2).reshape(*lead, rows // 8, cells // 16, 128)


def untiles(block):
    lead = block.shape[:-3]
    groups, wide, _ = block.shape[-3:]
    split = block.reshape(*lead, groups, wide // 8, 8, 128)
    return jnp.swapaxes(split, -3, -2).reshape(*lead, groups * 8, wide * 16)


def masks():
    sub = lax.broadcasted_iota(jnp.int32, (8, 128), 0)
    lane = lax.broadcasted_iota(jnp.int32, (8, 128), 1)
    first = lane == 0
    last = lane == 127
    return first, last, first & (sub == 0), last & (sub == 7)


def beside(row, m):
    first, last, left_end, right_end = m
    left = pltpu.roll(row, 1, 1)
    left = jnp.where(first, pltpu.roll(left, 1, 0), left)
    right = pltpu.roll(row, 127, 1)
    right = jnp.where(last, pltpu.roll(right, 7, 0), right)
    return jnp.where(left_end, 0.0, left) + jnp.where(right_end, 0.0, right)


def around(ref, row, m):
    return beside(ref[row], m) + (ref[row - 1] + ref[row + 1])


def loop(low, high, body, carry=None, unroll=4):
    quiet = carry is None
    steps = (high - low) // unroll

    def block(n, value):
        for k in range(unroll):
            value = (body(low + n * unroll + k), value)[1] if quiet else body(low + n * unroll + k, value)
        return value

    value = lax.fori_loop(0, steps, block, 0 if quiet else carry)
    for i in range(low + steps * unroll, high):
        value = (body(i), value)[1] if quiet else body(i, value)
    return None if quiet else value


BLOCK = 64


def padded(rows):
    return -(-(rows - 2) // BLOCK) * BLOCK + 2


def block_loop(low, high, body, carry, unroll):
    high = low + -(-(high - low) // unroll) * unroll
    return loop(low, high, body, carry, unroll)


def strided(ref, lead, row_group, k):
    return ref[lead + (row_group, pl.ds(k, 8, stride=8))]


def place_of():
    return lax.rem(lax.axis_index("tm"), TEAM)


def odd_strip():
    return lax.rem(lax.axis_index("space"), 2) == 1


def either(flag, body, one, two):
    pl.when(flag)(lambda: body(two, one))
    pl.when(jnp.logical_not(flag))(lambda: body(one, two))


def take_later(guess, out, *done):
    part = out.shape[0] // len(done)
    copies = []
    for k, sem in enumerate(done):
        at = pl.ds(k * part, part)
        copies.append(pltpu.make_async_copy(guess.at[1, at], out.at[at], sem))
    for copy in copies:
        copy.start()
    for copy in copies:
        copy.wait()


def pack_edges(g_top, r_top, d_top, g_end, r_end, d_end, pair, other):
    count = g_top.shape[1] * 8
    refs = [((g_top, (t,)), (g_end, (t,))) for t in range(2)]
    refs += [((r_top, (t,)), (r_end, (t,))) for t in range(2)]
    refs += [((d_top, ()), (d_end, ()))]

    def fill(end, top):
        for i, ((a, lead_a), (b, lead_b)) in enumerate(refs):
            for k in range(HALO):
                top[i * HALO + k] = strided(a, lead_a, k // 8, k % 8)
                row = count - HALO + k
                end[i * HALO + k] = strided(b, lead_b, row // 8, row % 8)

    either(odd_strip(), fill, pair, other)


def first_sweep(guess, rhs, diff, send, g1):
    rows = guess.shape[1] * 8
    m = masks()

    def unpack(g):
        for k in range(8):
            i = g * 8 + k
            g1[1 + i] = strided(guess, (1,), g, k)

    loop(0, rows // 8, unpack, unroll=2)

    def sweep(g):
        for k in range(8):
            i = g * 8 + k
            s = strided(diff, (), g, k)
            w = DAMPING / (1.0 + 4.0 * s)
            whole = strided(rhs, (1,), g, k) + s * around(g1, 1 + i, m) + strided(guess, (0,), g, k)
            send[i] = KEEP * g1[1 + i] + w * whole

    loop(0, rows // 8, sweep, unroll=4)


def local_parts(guess, rhs, diff, pair, other, s_ext, w_ext, part0, left0, left1, v1, edges, g0, g1, low, high, drift):
    rows = rhs.shape[1] * 8
    m = masks()

    def unpack(g):
        for k in range(8):
            i = HALO + g * 8 + k
            s = strided(diff, (), g, k)
            s_ext[i] = s
            w_ext[i] = DAMPING / (1.0 + 4.0 * s)
            g0[i] = strided(guess, (0,), g, k)
            g1[i] = strided(guess, (1,), g, k)

    def order(after, before):
        for k in range(5 * HALO):
            low[k] = before[k]
            high[k] = after[k]

    either(odd_strip(), order, pair, other)
    loop(0, rows // 8, unpack, unroll=2)
    for k in range(HALO):
        for dst, i in ((g0, 0), (g1, 1), (s_ext, 4)):
            dst[k] = low[i * HALO + k]
            dst[HALO + rows + k] = high[i * HALO + k]
        for i in (k, HALO + rows + k):
            w_ext[i] = DAMPING / (1.0 + 4.0 * s_ext[i])

    def fill(i, a, b):
        s = s_ext[i]
        w = w_ext[i]
        part0[i] = KEEP * g0[i] + w * (a + s * around(g0, i, m))
        v1[i] = KEEP * g1[i] + w * (b + s * around(g1, i, m) + g0[i])

    def inner(g):
        for k in range(8):
            fill(HALO + g * 8 + k, strided(rhs, (0,), g, k), strided(rhs, (1,), g, k))

    loop(0, rows // 8, inner, unroll=2)
    for k in range(1, HALO):
        fill(k, low[2 * HALO + k], low[3 * HALO + k])
    for k in range(0, HALO - 1):
        fill(HALO + rows + k, high[2 * HALO + k], high[3 * HALO + k])
    ends = [(2, HALO - 1), (HALO + rows, 2 * HALO + rows - 3)]
    for n, (first, final) in enumerate(ends):
        for i in range(first - 1, final + 2):
            drift[n * (SIDE + 1) + i - first + 1] = w_ext[i] * g1[i]
    for n, (first, final) in enumerate(ends):
        for i in range(first, final + 1):
            at = n * (SIDE + 1) + i - first + 1
            s = s_ext[i]
            here = drift[at]
            edges[n * (SIDE - 1) + i - first] = v1[i] - 4.0 * s * here + s * around(drift, at, m)
    low_at = 2 * (SIDE - 1)
    edges[low_at] = w_ext[HALO - 1] * g1[HALO - 1]
    edges[low_at + 1] = w_ext[HALO + rows] * g1[HALO + rows]
    edges[low_at + 2] = v1[HALO]
    edges[low_at + 3] = v1[HALO + rows - 1]

    def rest(i, a, b):
        s = s_ext[i]
        diag = 1.0 + 4.0 * s
        left0[i] = a - diag * part0[i] + s * around(part0, i, m)
        left1[i] = b - diag * v1[i] + s * around(v1, i, m) + part0[i]

    def inner2(g):
        for k in range(8):
            rest(HALO + g * 8 + k, strided(rhs, (0,), g, k), strided(rhs, (1,), g, k))

    loop(0, rows // 8, inner2, unroll=2)
    for k in range(2, HALO):
        rest(k, low[2 * HALO + k], low[3 * HALO + k])
    for k in range(0, HALO - 2):
        rest(HALO + rows + k, high[2 * HALO + k], high[3 * HALO + k])


def windows_of(rows):
    piece = -(-(rows + 2 * EDGE) // TEAM)
    spare = rows + 2 * EDGE - piece

    def start(j):
        return j * spare // (TEAM - 1) - EDGE

    return piece, piece + 2 * REACH, start


def join_first(start_of, window, g_prev, got, edges, s_ext, w_ext, left0, left1, *refs):
    outs = refs[:TEAM]
    y, resid0, coarse = refs[TEAM:]
    place = place_of()
    rows = got.shape[0]
    m = masks()

    def inner(g):
        for k in range(8):
            i = HALO + g * 8 + k
            y[i] = w_ext[i] * strided(g_prev, (), g, k)

    loop(0, rows // 8, inner, unroll=2)
    single = 2 * (SIDE - 1)
    y[HALO - 1] = edges[single]
    y[HALO + rows] = edges[single + 1]

    def resid(i, swept):
        s = s_ext[i]
        here = y[i]
        a = left0[i] - (1.0 + 4.0 * s) * here + s * around(y, i, m) + swept
        resid0[i] = a
        coarse[i] = a + left1[i] + here

    loop(HALO + 1, HALO + rows - 1, lambda i: resid(i, got[i - HALO]), unroll=32)
    resid(HALO, edges[single + 2])
    resid(HALO + rows - 1, edges[single + 3])
    for k in range(SIDE - 1):
        for i, at in ((2 + k, k), (HALO + rows + k, SIDE - 1 + k)):
            taken = left0[i] + edges[at]
            coarse[i] = taken + left1[i]
            if i in (HALO - 1, HALO + rows):
                resid0[i] = taken - y[i]
    for k, out in enumerate(outs):
        low = start_of(place ^ k) - REACH + HALO

        def copy(i, out=out, low=low):
            out[i] = coarse[low + i]

        loop(0, window, copy, unroll=16)


def join_rest(w_ext, part0, left1, v1, y, resid0, base0, base1, back, norm):
    rows = back.shape[0]

    def based(i):
        w = w_ext[i]
        a = resid0[i]
        b = left1[i] + y[i]
        base0[i - HALO + 1] = part0[i] + y[i] + w * a
        value = v1[i] + w * b
        base1[i - HALO + 1] = value
        return a, b, value

    def main(i, acc):
        a, b, value = based(i)
        back[i - HALO] = value
        return acc + (a * a + b * b)

    norm[...] = loop(HALO, HALO + rows, main, jnp.zeros((8, 128), jnp.float32), unroll=8)
    based(HALO - 1)
    based(HALO + rows)


def coarse_levels(start_of, rows, s_ext, *refs):
    g_in, refs = refs[:TEAM], refs[TEAM:]
    outs, refs = refs[:TEAM], refs[TEAM:]
    norms, s_win, w_win, v_ref, e_ref, final = refs[:6]
    bases = refs[6:]
    window = g_in[0].shape[0]
    piece = window - 2 * REACH
    m = masks()
    place = place_of()
    start = start_of(place) - REACH
    first_own = place * (rows // TEAM) - start
    last_own = first_own + rows // TEAM

    def level_weights(i):
        s = s_ext[start + HALO + i]
        s_win[i] = s
        for level in range(1, LEVELS):
            w_win[level - 1, i] = DAMPING / (1.0 + 4.0 * 2.0**level * s)

    loop(0, window, level_weights, unroll=12)

    def own(i, value):
        return jnp.where((i >= first_own) & (i < last_own), value, 0.0)

    source = None
    zero = jnp.zeros((8, 128), jnp.float32)
    for level in range(1, LEVELS - 1):
        points = TEAM >> (level - 1)
        lost = level - 1
        base = bases[2 * (level - 1)]
        target = bases[2 * (level - 1) + 1]

        def smooth(i, level=level, points=points, source=source):
            w = w_win[level - 1, i]
            for p in range(points):
                if source is None:
                    v_ref[place ^ p, i] = w * g_in[p][i]
                else:
                    v_ref[p, i] = w * source[p, i]

        loop(0, window, smooth, unroll=2)

        def descend(i, acc, level=level, points=points, source=source, base=base, target=target):
            s = 2.0**level * s_win[i]
            w = w_win[level - 1, i]
            pairs = []
            total = zero
            before = None
            for p in range(points):
                here = v_ref[p, i]
                r = 0.25 * here + s * (here + beside(here, m) + (v_ref[p, i - 1] + v_ref[p, i + 1]))
                if before is not None:
                    r = r + before
                base[p, i] = here + w * r
                total = total + r * r
                pairs.append(r)
                before = here
            for q in range(points // 2):
                target[q, i] = pairs[2 * q] + pairs[2 * q + 1]
            return acc + own(i, total)

        norms[level - 1] = block_loop(1, window - 1, descend, zero, BLOCK // points)
        source = target

    level = LEVELS - 1
    lost = level - 1

    def smooth_last(i):
        v_ref[0, i] = w_win[level - 1, i] * source[0, i]

    loop(0, window, smooth_last, unroll=16)

    def again(i):
        s = 2.0**level * s_win[i]
        here = v_ref[0, i]
        r = 0.25 * here + s * (here + beside(here, m) + (v_ref[0, i - 1] + v_ref[0, i + 1]))
        e_ref[0, i] = here + w_win[level - 1, i] * r

    block_loop(1, window - 1, again, None, BLOCK)

    def last_residual(i, acc):
        s = 2.0**level * s_win[i]
        here = e_ref[0, i]
        r = source[0, i] - (1.0 + 4.0 * s) * here
        r = r + s * (beside(here, m) + (e_ref[0, i - 1] + e_ref[0, i + 1]))
        return acc + own(i, r * r)

    norms[level - 1] = block_loop(1, window - 1, last_residual, zero, BLOCK)

    lost = LEVELS - 1
    field, other = e_ref, v_ref
    for level in range(LEVELS - 2, 0, -1):
        points = TEAM >> (level - 1)
        lost += 1
        base = bases[2 * (level - 1)]

        def ascend(i, level=level, points=points, base=base, field=field, other=other):
            s = 2.0**level * s_win[i]
            w = w_win[level - 1, i]
            before = None
            for q in range(points // 2):
                e = field[q, i]
                part = KEEP * e + w * (s * (beside(e, m) + (field[q, i - 1] + field[q, i + 1])))
                kept = w * e
                for p in (2 * q, 2 * q + 1):
                    value = base[p, i] + part
                    drift = before if p == 2 * q else kept
                    if drift is not None:
                        value = value + drift
                    if level == 1:
                        final[p + 1, i - REACH] = value
                    else:
                        other[p, i] = value
                before = kept

        span = BLOCK // points * 2
        if level == 1:
            loop(lost, window - lost, ascend, unroll=11)
        else:
            block_loop(1, window - 1, ascend, None, span)
        field, other = other, field

    def blank(i):
        final[0, i] = zero

    loop(0, piece, blank, unroll=11)
    for k, out in enumerate(outs):

        target = place ^ k
        odd = lax.rem(target, 2)
        half = out.shape[0] - piece

        def copy(i, out=out, at=target + odd):
            out[i] = final[at, i]

        def copy_half(i, out=out, at=target - odd + 1, skip=odd * (piece - half), half=half):
            out[piece + i] = final[at, skip + i]

        loop(0, piece, copy, unroll=11)
        loop(0, half, copy_half, unroll=17)


def odd_place():
    return lax.rem(lax.axis_index("tm"), 2)


def pick_halves(piece, *refs):
    fields, (out,) = refs[:TEAM], refs[TEAM:]
    half = fields[0].shape[0] - piece
    place = place_of()
    for k, got in enumerate(fields):
        first = (place ^ k) * half

        def copy(i, got=got, first=first):
            out[first + i] = got[piece + i]

        loop(0, half, copy, unroll=17)


def spread(field, s_ext, w_ext, out):
    m = masks()

    def body(i):
        s = s_ext[i + HALO - 1]
        out[i] = KEEP * field[i + 1] + w_ext[i + HALO - 1] * (s * around(field, i + 1, m))

    loop(0, out.shape[0], body, unroll=43)


def spread_own(start_of, piece, s_ext, w_ext, *refs):
    fields, (own, out) = refs[:TEAM], refs[TEAM:]
    place = place_of()
    for k, got in enumerate(fields):
        start = start_of(place ^ k) + EDGE

        def copy(i, got=got, start=start):
            own[start + i] = got[i]

        loop(0, piece, copy, unroll=11)
    spread(own, s_ext, w_ext, out)


def finish(start_of, piece, rhs, s_ext, w_ext, base0, base1, own, own_spread, halves, *refs):
    fields = refs[:TEAM]
    whole, left, norm, shared, shared_spread, sol0, sol1, out, *done = refs[TEAM:]
    groups = rhs.shape[1]
    share = groups // len(done)
    rows = rhs.shape[1] * 8
    half = fields[0].shape[0] - piece
    m = masks()
    place = place_of()
    odd = odd_place()
    skip = odd * (piece - half)
    for k, got in enumerate(fields):
        start = start_of(place ^ k) + EDGE + skip

        def copy(i, got=got, start=start):
            shared[start + i] = got[piece + i]

        loop(0, half, copy, unroll=17)
    for j in range(TEAM):
        start = start_of(j) + EDGE + (piece - half) - skip

        def copy(i, j=j, start=start):
            shared[start + i] = halves[j * half + i]

        loop(0, half, copy, unroll=17)
    spread(shared, s_ext, w_ext, shared_spread)

    def solve(now, before):
        e, part = now
        past, past_part = before

        def correct(i):
            w = w_ext[i + HALO - 1]
            sol0[i] = base0[i] + part[i] + w * past[i + 1]
            sol1[i] = base1[i] + part[i] + w * e[i + 1]

        loop(0, rows + 2, correct, unroll=8)

        def last(g, acc):
            for k in range(8):
                i = g * 8 + k
                s = s_ext[i + HALO]
                diag = 1.0 + 4.0 * s
                older = past_part[i + 1] + w_ext[i + HALO] * past[i + EDGE]
                a = sol0[i + 1]
                b = sol1[i + 1]
                left[i] = strided(rhs, (0,), g, k) - diag * a + s * around(sol0, i + 1, m) + older
                rb = strided(rhs, (1,), g, k) - diag * b + s * around(sol1, i + 1, m) + a
                out[0, g, pl.ds(k, 8, stride=8)] = a
                out[1, g, pl.ds(k, 8, stride=8)] = b
                acc = acc + rb * rb
            return acc

        acc = jnp.zeros((8, 128), jnp.float32)
        copies = []
        for n, sem in enumerate(done):
            acc = loop(n * share, (n + 1) * share, last, acc, unroll=4)
            at = pl.ds(n * share, share)
            copies.append(pltpu.make_async_copy(out.at[:, at], whole.at[:, at], sem))
            copies[-1].start()
        norm[...] = acc
        for copy in copies:
            copy.wait()

    either(odd == 1, solve, (shared, shared_spread), (own, own_spread))


def add_up(left, back, norm0, norms, norm, sums):
    def body(i, acc):
        r = left[i] + back[i]
        return acc + r * r

    acc = loop(0, back.shape[0], body, norm[...], unroll=16)
    parts = [norm0[...]] + [norms[k] for k in range(LEVELS - 1)] + [acc]
    for k, part in enumerate(parts):
        sums[pl.ds(k, 1)] = jnp.sum(part, axis=0, keepdims=True)
    for k in range(len(parts), 8):
        sums[pl.ds(k, 1)] = jnp.zeros((1, 128), jnp.float32)


def coarse_plain(g_in, s_win, own, earlier):
    cells = g_in.shape[-2] * 128

    def flat(x):
        return x.reshape(*x.shape[:-2], cells)

    def around_plain(v):
        padded = jnp.pad(v, ((0, 0), (1, 1), (1, 1)))
        total = padded[:, 2:, 1:-1] + padded[:, :-2, 1:-1]
        return total + padded[:, 1:-1, 2:] + padded[:, 1:-1, :-2]

    def resid(v, g, s, before):
        past = jnp.concatenate([before, v[:-1]], axis=0)
        return g - (1.0 + 4.0 * s) * v + s * around_plain(v) + past

    source = flat(g_in)
    s_win = flat(s_win)
    sources, fields, norms = [], [], []
    for level in range(1, LEVELS):
        s = 2.0**level * s_win
        w = DAMPING / (1.0 + 4.0 * s)
        v = w * source
        r = resid(v, source, s, earlier(v[-1:]))
        if level == LEVELS - 1:
            v = v + w * r
            r = resid(v, source, s, earlier(v[-1:]))
        masked = jnp.where(own[None, :, None], r, 0.0)
        norms.append((masked * masked).reshape(-1, 8, 128).sum(0))
        sources.append(source)
        fields.append(v)
        if level < LEVELS - 1:
            source = r[0::2] + r[1::2]
    field = fields[-1]
    for level in range(LEVELS - 2, 0, -1):
        s = 2.0**level * s_win
        w = DAMPING / (1.0 + 4.0 * s)
        field = fields[level - 1] + jnp.repeat(field, 2, axis=0)
        field = field + w * resid(field, sources[level - 1], s, earlier(field[-1:]))
    past = jnp.concatenate([earlier(field[-1:]), field[:-1]], axis=0)
    field, past = [x[:, REACH : x.shape[1] - REACH] for x in (field, past)]
    half = -(-field.shape[1] // 2)
    even = jnp.concatenate([past, field[:, :half]], axis=1)
    odd = jnp.concatenate([field, past[:, -half:]], axis=1)
    both = jnp.where((jnp.arange(TEAM) % 2 == 1)[:, None, None], odd, even)
    return both.reshape(*both.shape[:2], 8, 128), jnp.stack(norms)


def body(count, strips, rhs, guess, diffusion):
    points, rows, cells = rhs.shape
    assert points == 2 and cells == 1024 and count % TEAM == 0
    assert rows % (8 * TEAM) == 0
    total_cells = rows * strips * cells
    groups = rows // 8
    piece, window, start_of = windows_of(rows)
    half_piece = -(-piece // 2)
    wide = cells // 16
    ext = rows + 2 * HALO

    def both(first):
        pairs = [(i, i + 1) for i in range(first, strips - 1, 2)]
        return pairs + [(b, a) for a, b in pairs]

    later = [(i, i + 1) for i in range(count - 1)]

    rhs_t, guess_t, diff_t = tiles(rhs), tiles(guess), tiles(diffusion)
    edge_groups = -(-HALO // 8)
    assert groups % edge_groups == 0
    far = groups // edge_groups - 1

    def edge_specs(block):
        time = pl.BlockSpec((2, edge_groups, wide, 128), lambda i: (0, block, 0, 0))
        flat = pl.BlockSpec((edge_groups, wide, 128), lambda i: (block, 0, 0))
        return [time, time, flat]

    far_args = [pltpu.with_memory_space_constraint(x, pltpu.HBM) for x in (guess_t, rhs_t, diff_t)]
    (g_prev,) = kernel_call(
        take_later,
        [shape(groups, wide, 128)],
        specs=[pl.BlockSpec(memory_space=pl.ANY)],
        more=[pltpu.SemaphoreType.DMA(())] * 4,
    )(far_args[0])
    g_prev = lax.ppermute(g_prev, "tm", later)
    facing, backing = kernel_call(
        pack_edges, [shape(5 * HALO, 8, 128)] * 2, specs=edge_specs(0) + edge_specs(far), grid=(1,)
    )(*far_args, *far_args)
    facing = lax.ppermute(facing, "space", both(0))
    backing = lax.ppermute(backing, "space", both(1))
    (send,) = kernel_call(first_sweep, [shape(rows, 8, 128)], scratch=[(rows + 2, 8, 128)], n_in=3)(
        guess_t, rhs_t, diff_t
    )
    got = lax.ppermute(send, "tm", later)
    s_ext, w_ext, part0, left0, left1, v1, edges = kernel_call(
        local_parts,
        [kept(ext, 8, 128)] * 2 + [shape(ext, 8, 128)] * 4 + [shape(2 * SIDE + 2, 8, 128)],
        scratch=[(ext, 8, 128)] * 2 + [(5 * HALO, 8, 128)] * 2 + [(2 * (SIDE + 1), 8, 128)],
        n_in=5,
    )(guess_t, rhs_t, diff_t, facing, backing)
    edges = lax.ppermute(edges, "tm", later)
    *mine, y, resid0 = kernel_call(
        functools.partial(join_first, start_of, window),
        [shape(window, 8, 128)] * TEAM + [shape(ext, 8, 128)] * 2,
        scratch=[(ext, 8, 128)],
        n_in=7,
    )(g_prev, got, edges, s_ext, w_ext, left0, left1)

    def exchange(order, parts):
        moved = list(parts)
        for k in order:
            moved[k] = lax.ppermute(parts[k], "tm", [(i, i ^ k) for i in range(count)])
        return moved

    mine = exchange(DOWN, mine)
    base0, base1, back, norm0 = kernel_call(
        join_rest,
        [kept(rows + 2, 8, 128)] * 2 + [shape(rows, 8, 128), shape(8, 128)],
        n_in=6,
    )(w_ext, part0, left1, v1, y, resid0)
    back = lax.ppermute(back, "tm", later)
    if count == TEAM:
        tall = padded(window)
        half = [(TEAM >> level, tall, 8, 128) for level in range(LEVELS)]
        bases = []
        for level in range(1, LEVELS - 1):
            bases += [half[level - 1], half[level]]
        *fields, norms = kernel_call(
            functools.partial(coarse_levels, start_of, rows),
            [shape(piece + half_piece, 8, 128)] * TEAM + [shape(LEVELS - 1, 8, 128)],
            scratch=[(tall, 8, 128), (LEVELS - 1, tall, 8, 128), half[0], half[0], (TEAM + 1, piece, 8, 128)] + bases,
            n_in=1 + TEAM,
        )(s_ext, *mine)
    else:
        place = place_of()
        order = place ^ jnp.arange(TEAM)
        start = start_of(place) - REACH
        s_win = lax.dynamic_slice_in_dim(s_ext, start + HALO, window, axis=0)
        at = start + jnp.arange(window) - place * (rows // TEAM)
        own = (at >= 0) & (at < rows // TEAM)
        jumps = [(i, i + TEAM) for i in range(count - TEAM)]
        fields, norms = coarse_plain(jnp.stack(mine)[order], s_win, own, lambda v: lax.ppermute(v, "tm", jumps))
        fields = list(fields[order])
    fields = exchange(UP, fields)

    s_ext, w_ext, base0, base1 = keep(s_ext, w_ext, base0, base1)
    (halves,) = kernel_call(
        functools.partial(pick_halves, piece), [shape(TEAM * half_piece, 8, 128)], n_in=TEAM
    )(*fields)
    halves = lax.ppermute(halves, "tm", [(i, i ^ 1) for i in range(count)])
    own, own_spread = kernel_call(
        functools.partial(spread_own, start_of, piece),
        [shape(rows + 2 * EDGE, 8, 128), shape(rows + 2, 8, 128)],
        n_in=2 + TEAM,
    )(s_ext, w_ext, *fields)
    out, left, norm = kernel_call(
        functools.partial(finish, start_of, piece),
        [shape(2, groups, wide, 128), shape(rows, 8, 128), shape(8, 128)],
        scratch=[(rows + 2 * EDGE, 8, 128)] + [(rows + 2, 8, 128)] * 3 + [(2, groups, wide, 128)],
        more=[pltpu.SemaphoreType.DMA(())] * 8,
        out_specs=[pl.BlockSpec(memory_space=pl.ANY), vmem(), vmem()],
        n_in=8 + TEAM,
    )(rhs_t, s_ext, w_ext, base0, base1, own, own_spread, halves, *fields)
    (sums,) = kernel_call(add_up, [shape(8, 128)], n_in=5)(left, back, norm0, norms, norm)

    every = jnp.broadcast_to(sums[None], (count * strips, 8, 128))
    every = lax.all_to_all(every, ("tm", "space"), 0, 0)
    totals = every.sum(axis=(0, 2))[: LEVELS + 1]
    return untiles(out), jnp.sqrt(totals / total_cells)


def solution(mesh):
    in_specs = (P("tm", "space", None), P("tm", "space", None), P("space", None))
    out_specs = (P("tm", "space", None), P())
    step = functools.partial(body, mesh.shape["tm"], mesh.shape["space"])
    step = jax.shard_map(step, mesh=mesh, in_specs=in_specs, out_specs=out_specs, check_vma=False)
    return step
```
